256 devices in a mesh: gz: 32 (over z, x_lo, core), gx: 2 (over x_hi), gy: 4 (over y).
Axes of the slice: x: 4 (x_hi: 2, x_lo: 2; x = x_hi * 2 + x_lo), y: 4, z: 8, core: 2. Of those that a mesh axis runs over, the one named last changes fastest.
Arguments:
- density: float32 [128, 256, 4096], P('gx', 'gy', 'gz'), may hold values from 0.01 to 1
- design_mask: int32 [128, 256, 4096], P('gx', 'gy', 'gz'), may hold values from 0 to 2
- energy: bfloat16 [4, 128, 256, 4096], P(None, 'gx', 'gy', 'gz'), may hold values from 0.099609375 to 3
- decay: float32 [4, 4096], P(None, 'gz'), may hold values from 0.3 to 1
- case_index: int32 [4], replicated, may hold values from 0 to 15
- case_weight: float32 [16], replicated, may hold values from 0.2 to 1
Outputs:
- sensitivity: float32 [128, 256, 4096], P('gx', 'gy', 'gz')
- compliance: float32 [4], replicated
The draws below stay inside these ranges and needn't reach their ends.
All inputs are finite; a program needn't handle non-finite values.
Results may differ from the reference program's by a relative error of at most 0.0006.
Values may be sent and summed in bfloat16 or wider, within the bound.
A program may use at most 128 MiB of HBM per device.

```python
import math
import jax
import jax.numpy as jnp
from jax import lax

CASES = 4
LOADS = 16
RADIUS = 3
NX = 128
NY = 256
NZ = 4096


def draw_decay(key, part):
    key_order = jax.random.fold_in(key, 11)
    key_rough = jax.random.fold_in(key, 12)
    key_where = jax.random.fold_in(key, 13)
    key_depth = jax.random.fold_in(key, 14)
    order = jax.random.permutation(key_order, CASES)
    slow_case = order < (CASES + 1) // 2
    rough = jax.random.uniform(key_rough, (CASES, NZ), jnp.float32, 0.5, 1.5)
    slow_rate = jnp.log(1.0 / 0.3) / NZ
    rates = jnp.where(slow_case, slow_rate, 1.0 / 40.0).astype(jnp.float32)
    retained = jnp.exp(-rates[:, None] * rough)
    positions = jax.random.randint(key_where, (CASES, 2), 0, NZ)
    depths = jax.random.uniform(key_depth, (CASES, 2), jnp.float32, 0.55, 0.8)
    cells = jnp.arange(NZ)[None, :]
    factor = jnp.where(cells == positions[:, 0:1], depths[:, 0:1], 1.0)
    factor = factor * jnp.where(cells == positions[:, 1:2], depths[:, 1:2], 1.0)
    return (retained * factor).astype(jnp.float32)


def with_ends(result, key, smallest, top_value):
    dims = result.shape
    index_at = [jax.random.randint(jax.random.fold_in(key, axis), (), 0, dims[axis]) for axis in range(len(dims))]
    result = result.at[tuple(index_at)].set(smallest)
    longest = dims.index(max(dims))
    index_at[longest] = (index_at[longest] + 1) % dims[longest]
    return result.at[tuple(index_at)].set(top_value)


def steps_of(own_key, extent, shards, smallest, largest):
    gain = 1.0
    for axis_at, parts in shards:
        steps = jax.random.uniform(jax.random.fold_in(jax.random.fold_in(own_key, 6), axis_at), (parts,), jnp.float32, smallest / len(shards), largest / len(shards))
        gain = gain * jnp.repeat(jnp.exp(steps), extent[axis_at] // parts).reshape((-1,) + (1,) * (len(extent) - 1 - axis_at))
    return gain


def setup_inputs(seed: int = 0) -> dict:
    key_of = jax.random.split(jax.random.key(seed), 7)
    density = jnp.clip(jnp.exp(math.log(1.0) - 4.6051702 * jax.random.uniform(key_of[0], (NX, NY, NZ), jnp.float32) ** steps_of(key_of[0], (NX, NY, NZ), ((0, 2), (1, 4), (2, 32)), -0.2, 0.2)), 0.01, 1.0)
    design_mask = with_ends(jax.random.randint(key_of[1], (NX, NY, NZ), 0, 3), jax.random.fold_in(key_of[1], 1), 0, 2).astype(jnp.int32)
    energy = jnp.clip(jnp.exp(math.log(3.0) - 3.4051113 * jax.random.uniform(key_of[2], (CASES, NX, NY, NZ), jnp.float32) ** steps_of(key_of[2], (CASES, NX, NY, NZ), ((1, 2), (2, 4), (3, 32)), -0.2, 0.2)), 0.099609375, 3.0).astype(jnp.bfloat16)
    decay = draw_decay(jax.random.fold_in(key_of[6], 71), 0)
    case_index = with_ends(jax.random.randint(key_of[4], (CASES,), 0, LOADS), jax.random.fold_in(key_of[4], 1), 0, LOADS - 1).astype(jnp.int32)
    case_weight = jnp.clip(jax.random.uniform(key_of[5], (LOADS,), jnp.float32, 0.2, 1.0), 0.2, 1.0)
    return dict(density=density, design_mask=design_mask, energy=energy, decay=decay, case_index=case_index, case_weight=case_weight)


def kernel_taps():
    offsets = jnp.arange(-RADIUS, RADIUS + 1).astype(jnp.float32)
    raw_taps = jnp.exp(-2.0 * offsets * offsets / (RADIUS * RADIUS))
    return raw_taps / jnp.sum(raw_taps)


def planar_filter(padded, width_x, width_y):
    taps = kernel_taps()
    along_x = taps[0] * padded[:, 0:width_x]
    for offset in range(1, 2 * RADIUS + 1):
        along_x = along_x + taps[offset] * padded[:, offset:offset + width_x]
    along_y = taps[0] * along_x[:, :, 0:width_y]
    for offset in range(1, 2 * RADIUS + 1):
        along_y = along_y + taps[offset] * along_x[:, :, offset:offset + width_y]
    return along_y


def solid_density(density, design_mask):
    return jnp.where(design_mask == 1, 0.001, jnp.where(design_mask == 2, 1.0, density)).astype(jnp.float32)


def smooth_step(state, inputs):
    values, rate = inputs
    state = rate[:, None, None] * state + (1.0 - rate)[:, None, None] * values
    return state, state


def reference(density, design_mask, energy, decay, case_index, case_weight):
    dense = solid_density(density, design_mask)
    source = -3.0 * (dense ** 3)[None] * energy.astype(jnp.float32)
    padded = jnp.pad(source, ((0, 0), (RADIUS, RADIUS), (RADIUS, RADIUS), (0, 0)))
    planar = planar_filter(padded, NX, NY)
    columns = jnp.moveaxis(planar, 3, 0)
    rates = jnp.transpose(decay)
    initial = jnp.zeros((CASES, NX, NY), jnp.float32)
    _, forward = lax.scan(smooth_step, initial, (columns, rates))
    _, backward = lax.scan(smooth_step, initial, (forward, rates), reverse=True)
    smooth = jnp.moveaxis(backward, 0, 3)
    filtered = smooth / jnp.maximum(dense, 0.1)[None]
    selector = (case_index[:, None] == jnp.arange(LOADS).astype(jnp.int32)[None, :]).astype(jnp.float32)
    weights = jnp.sum(selector * case_weight[None, :], axis=1)
    combined = jnp.sum(weights[:, None, None, None] * filtered, axis=0)
    sensitivity = jnp.where(design_mask == 0, combined, 0.0).astype(jnp.float32)
    compliance = jnp.sum((dense ** 3)[None] * energy.astype(jnp.float32), axis=(1, 2, 3)) / (NX * NY * NZ)
    return sensitivity, compliance
```

```python
import functools
import math

import jax
import jax.numpy as jnp
from jax import lax
from jax.experimental import pallas as pl
from jax.experimental.pallas import tpu as pltpu
from jax.sharding import PartitionSpec as P

CASES = 4
RADIUS = 3
F32 = jnp.float32
BF16 = jnp.bfloat16
MESH = pl.DeviceIdType.MESH
HIGH = lax.Precision.HIGHEST
XG = 8
YO = 8

_raw = [math.exp(-2.0 * k * k / (RADIUS * RADIUS)) for k in range(-RADIUS, RADIUS + 1)]
TAPS = [t / sum(_raw) for t in _raw]


def dot(a, b, ca, cb, precision=None):
    return lax.dot_general(a, b, (((ca,), (cb,)), ((), ())), precision=precision, preferred_element_type=F32)


def split(value):
    hi = value.astype(BF16)
    return hi, (value - hi.astype(F32)).astype(BF16)


def kernel(
    sizes, dens_hbm, mask_hbm, en_hbm, decay_ref, index_ref, weight_ref,
    out_hbm, comp_out,
    dens, mask, en, scale, lhs, maps, coef, vmap, ext, tmp, out,
    consts_out, consts_in, fh_out, fh_in, fin, carry_out, carry_in,
    cs_out, cs_in, ct_out, ct_in, xs_out, xs_in, ys_out, ys_in, ds_out, ds_in,
    load_sem, out_sem, cst_s, cst_r, ph1_s, ph1_r, ph2_s, ph2_r, cs_s, cs_r, ct_s, ct_r,
    xs_s, xs_r, ys_s, ys_r, ds_s, ds_r,
):
    n, ngx, ngy, lx, ly, lz, cells = sizes
    groups = lx // XG
    per = XG * ly
    gz, gx, gy = lax.axis_index("gz"), lax.axis_index("gx"), lax.axis_index("gy")
    others = ngx * ngy - 1

    def peer(k):
        flat = lax.rem(gx * ngy + gy + 1 + k, ngx * ngy)
        return {"gz": gz, "gx": flat // ngy, "gy": lax.rem(flat, ngy)}

    barrier = pltpu.get_barrier_semaphore()

    def greet(k, _):
        pl.semaphore_signal(barrier, inc=1, device_id={"gz": lax.rem(gz + k, n)}, device_id_type=MESH)
        return 0

    lax.fori_loop(1, n, greet, 0)
    for k in range(others):
        pl.semaphore_signal(barrier, inc=1, device_id=peer(k), device_id_type=MESH)

    def loads(k):
        rows = pl.ds(k * XG, XG)
        return (
            pltpu.make_async_copy(dens_hbm.at[rows], dens.at[rows], load_sem.at[0, k]),
            pltpu.make_async_copy(mask_hbm.at[rows], mask.at[rows], load_sem.at[1, k]),
            pltpu.make_async_copy(en_hbm.at[:, rows], en.at[:, rows], load_sem.at[2, k]),
        )

    def start_loads(k, _):
        for copy in loads(k):
            copy.start()
        return 0

    lax.fori_loop(0, groups, start_loads, 0)

    decay = jnp.concatenate([decay_ref[...], decay_ref[...]], axis=0)
    logs = jnp.log(decay)
    row = lax.broadcasted_iota(jnp.int32, (lz, lz), 0)
    col = lax.broadcasted_iota(jnp.int32, (lz, lz), 1)
    up = dot(logs, (row <= col).astype(F32), 1, 0, HIGH)
    down = dot(logs, (row >= col).astype(F32), 1, 0, HIGH)
    keep = 1.0 - decay
    columns = jnp.transpose(jnp.concatenate([up, down, keep, keep], axis=0))
    total = up[:, lz - 1 : lz]
    fwd_last = jnp.exp(total - up) * keep
    first = jnp.exp(down[:, 0:1] - down) * keep
    lead = jnp.exp(up)
    trail = jnp.exp(down)
    maps[...] = jnp.zeros_like(maps)
    coef[...] = jnp.zeros_like(coef)
    rows8 = lax.broadcasted_iota(jnp.int32, (8, lz), 0)
    cblock = jnp.zeros((8, lz), F32)
    vals = jnp.zeros((8, lz), F32)
    couple = jnp.zeros((8, lz), F32)
    for c in range(CASES):
        wc = weight_ref[index_ref[c]] * -3.0
        up_col, down_col, keep_col = columns[:, c : c + 1], columns[:, 8 + c : 9 + c], columns[:, 16 + c : 17 + c]
        low = row <= col
        fwd_t = jnp.where(low, jnp.exp(jnp.where(low, up[c : c + 1] - up_col, 0.0)), 0.0) * keep_col
        high = row >= col
        bwd_t = jnp.where(high, jnp.exp(jnp.where(high, down[c : c + 1] - down_col, 0.0)), 0.0) * keep_col
        both = dot(fwd_t, bwd_t, 1, 0, HIGH) * wc
        hi, lo = split(both)
        for half in range(2):
            at = (2 * c + half) * lz
            maps[at : at + lz, 0:lz] = hi
            maps[at : at + lz, lz : 2 * lz] = lo
        hrow = dot(first, fwd_t, 1, 1, HIGH)
        lead_map = dot(lead, bwd_t, 1, 0, HIGH)
        cblock = jnp.where(rows8 == c, fwd_last, 0.0)
        cblock = jnp.where(rows8 == c + CASES, hrow, cblock)
        chi = cblock.astype(BF16).astype(F32)
        pair = jnp.concatenate([chi, cblock - chi], axis=0).astype(BF16)
        for half in range(2):
            at = (2 * c + half) * lz
            coef[:, at : at + lz] = pair
        vals = jnp.where(rows8 == c, lead_map * wc, vals)
        vals = jnp.where(rows8 == c + CASES, trail * wc, vals)
        couple = jnp.where((rows8 == c) | (rows8 == c + CASES), jnp.broadcast_to(lead_map[:, 0:1], (8, lz)), couple)
    vhi = vals.astype(BF16).astype(F32)
    vmap[...] = jnp.concatenate([vhi, vhi, vals - vhi, jnp.zeros((8, lz), F32)], axis=0).astype(BF16)
    consts_out[0:8] = jnp.broadcast_to(jnp.exp(total), (8, lz))
    consts_out[8:16] = couple
    consts_in[gz] = consts_out[...]

    pl.semaphore_wait(barrier, n - 1 + others)

    def to_slab(src, dst, send, recv, k):
        return pltpu.make_async_remote_copy(
            src_ref=src, dst_ref=dst, send_sem=send, recv_sem=recv,
            device_id={"gz": k}, device_id_type=MESH,
        )

    def consts_copy(src, dst):
        return to_slab(consts_out, consts_in.at[src], cst_s.at[dst], cst_r.at[src], dst)

    def ph1_copy(src, dst):
        return to_slab(fh_out.at[dst], fh_in.at[src], ph1_s.at[dst], ph1_r.at[src], dst)

    def ph2_copy(src, dst):
        return to_slab(carry_out.at[dst], carry_in.at[src], ph2_s.at[dst], ph2_r.at[src], dst)

    def ct_copy(src, dst):
        return to_slab(ct_out, ct_in.at[src], ct_s.at[dst], ct_r.at[src], dst)

    def send_consts(k, _):
        consts_copy(gz, lax.rem(gz + k, n)).start()
        return 0

    lax.fori_loop(1, n, send_consts, 0)

    ext[...] = jnp.zeros_like(ext)

    def local(k, sums):
        for copy in loads(k):
            copy.wait()
        sums = list(sums)
        for i in range(XG):
            x = k * XG + i
            d, m = dens[x], mask[x]
            dense = jnp.where(m == 1, 0.001, jnp.where(m == 2, 1.0, d))
            cube = dense * dense * dense
            scale[x] = jnp.where(m == 0, 1.0 / jnp.maximum(d, 0.1), 0.0)
            for c in range(CASES):
                g = cube * en[c, x].astype(F32)
                sums[c] = sums[c] + jnp.sum(g.reshape(ly // 8, 8, lz), axis=0)
                hi, lo = split(g)
                lhs[i * ly : (i + 1) * ly, 2 * c * lz : (2 * c + 1) * lz] = hi
                lhs[i * ly : (i + 1) * ly, (2 * c + 1) * lz : (2 * c + 2) * lz] = lo
        full = dot(lhs[...], maps[...], 1, 0)
        full = full[:, :lz] + full[:, lz:]
        ext[pl.ds(RADIUS + k * XG, XG), YO : YO + ly, :] = full.reshape(XG, ly, lz)
        fh = dot(coef[...], lhs[...], 1, 1)
        fh = fh[0:8] + fh[8:16]
        for b in range(per // lz):
            p = k * (per // lz) + b
            fh_out[p] = fh[:, b * lz : (b + 1) * lz]
        return tuple(sums)

    sums = lax.fori_loop(0, groups, local, tuple(jnp.zeros((8, lz), F32) for _ in range(CASES)))

    def send_ph1(k, _):
        ph1_copy(gz, lax.rem(gz + k, n)).start()
        return 0

    lax.fori_loop(1, n, send_ph1, 0)
    fh_in[gz] = fh_out[gz]

    cs_out[...] = jnp.concatenate([jnp.sum(s, axis=0, keepdims=True) for s in sums] * 2, axis=0)

    def cs_copy(k):
        return pltpu.make_async_remote_copy(
            src_ref=cs_out, dst_ref=cs_in.at[k], send_sem=cs_s.at[k], recv_sem=cs_r.at[k],
            device_id=peer(k), device_id_type=MESH,
        )

    for k in range(others):
        cs_copy(k).start()
    part = cs_out[...]
    for k in range(others):
        cs_copy(k).wait_recv()
        part = part + cs_in[k]
    ct_out[...] = part

    def send_ct(k, _):
        ct_copy(gz, lax.rem(gz + k, n)).start()
        return 0

    lax.fori_loop(1, n, send_ct, 0)
    ct_in[gz] = part

    def ascend(s, state):
        @pl.when(s != gz)
        def _():
            consts_copy(s, gz).wait_recv()
            ph1_copy(s, gz).wait_recv()

        fin[s] = state
        return consts_in[s, 0:8] * state + fh_in[s]

    lax.fori_loop(0, n, ascend, jnp.zeros((8, lz), F32))

    def descend(k, state):
        s = n - 1 - k
        entering = fin[s]
        carry_out[s] = jnp.where(rows8 < CASES, entering, state)

        @pl.when(s != gz)
        def _():
            ph2_copy(gz, s).start()

        turned = pltpu.roll(entering, CASES, 0)
        return consts_in[s, 0:8] * state + fh_in[s] + consts_in[s, 8:16] * turned

    lax.fori_loop(0, n, descend, jnp.zeros((8, lz), F32))
    carry_in[gz] = carry_out[gz]

    rows_per = lz // ly

    def correct(p, _):
        @pl.when(p != gz)
        def _():
            ph2_copy(p, gz).wait_recv()

        state = carry_in[p]
        hi = state.astype(BF16).astype(F32)
        stack = jnp.concatenate([hi, state - hi, hi, jnp.zeros((8, lz), F32)], axis=0)
        add = dot(jnp.transpose(stack).astype(BF16), vmap[...], 1, 0)
        at = pl.ds(RADIUS + p * rows_per, rows_per)
        ext[at, YO : YO + ly, :] = ext[at, YO : YO + ly, :] + add.reshape(rows_per, ly, lz)
        return 0

    lax.fori_loop(0, n, correct, 0)

    xs_at = jnp.where(gx == 0, lx - RADIUS, 0)
    for j in range(RADIUS):
        xs_out[j] = ext[RADIUS + xs_at + j, YO : YO + ly, :].astype(BF16)
    for side in range(2):
        for j in range(RADIUS):
            y = YO + (j if side == 0 else ly - RADIUS + j)
            ys_out[side, j] = ext[RADIUS : RADIUS + lx, y, :].astype(BF16)
            ds_out[side, j] = ext[pl.ds(RADIUS + xs_at, RADIUS), y, :].astype(BF16)

    x_copy = pltpu.make_async_remote_copy(
        src_ref=xs_out, dst_ref=xs_in, send_sem=xs_s, recv_sem=xs_r,
        device_id={"gx": 1 - gx}, device_id_type=MESH,
    )

    def y_copy(side, to):
        return pltpu.make_async_remote_copy(
            src_ref=ys_out.at[side], dst_ref=ys_in.at[1 - side], send_sem=ys_s.at[side], recv_sem=ys_r.at[1 - side],
            device_id={"gy": to}, device_id_type=MESH,
        )

    def d_copy(side, to):
        return pltpu.make_async_remote_copy(
            src_ref=ds_out.at[side], dst_ref=ds_in.at[1 - side], send_sem=ds_s.at[side], recv_sem=ds_r.at[1 - side],
            device_id={"gx": 1 - gx, "gy": to}, device_id_type=MESH,
        )

    x_copy.start()

    @pl.when(gy > 0)
    def _():
        y_copy(0, gy - 1).start()
        d_copy(0, gy - 1).start()

    @pl.when(gy < ngy - 1)
    def _():
        y_copy(1, gy + 1).start()
        d_copy(1, gy + 1).start()

    def add_ct(s, state):
        @pl.when(s != gz)
        def _():
            ct_copy(s, gz).wait_recv()

        return state + ct_in[s]

    whole = lax.fori_loop(0, n, add_ct, jnp.zeros((8, lz), F32))
    for c in range(CASES):
        comp_out[c] = jnp.sum(whole[c : c + 1]) * (1.0 / cells)

    halo_x = jnp.where(gx == 0, RADIUS + lx, 0)
    x_copy.wait()
    ext[pl.ds(halo_x, RADIUS), YO : YO + ly, :] = xs_in[...].astype(F32)

    def take(side):
        for j in range(RADIUS):
            y = YO + (j - RADIUS if side == 0 else ly + j)
            ext[RADIUS : RADIUS + lx, y, :] = ys_in[side, j].astype(F32)
            ext[pl.ds(halo_x, RADIUS), y, :] = ds_in[side, j].astype(F32)

    @pl.when(gy > 0)
    def _():
        for copy in (y_copy, d_copy):
            copy(0, gy - 1).wait_send()
            copy(1, gy - 1).wait_recv()
        take(0)

    @pl.when(gy < ngy - 1)
    def _():
        for copy in (y_copy, d_copy):
            copy(1, gy + 1).wait_send()
            copy(0, gy + 1).wait_recv()
        take(1)

    def out_copy(k):
        rows = pl.ds(k * XG, XG)
        return pltpu.make_async_copy(out.at[rows], out_hbm.at[rows], out_sem.at[k])

    def taps(get):
        acc = TAPS[RADIUS] * get(RADIUS)
        for t in range(RADIUS):
            acc = acc + TAPS[t] * (get(t) + get(2 * RADIUS - t))
        return acc

    def filtered(k, _):
        for i in range(XG):
            x = k * XG + i
            tmp[i] = taps(lambda t: ext[x + t])
            along = taps(lambda t: tmp[i, YO - RADIUS + t : YO - RADIUS + t + ly, :])
            out[x] = along * scale[x]
        out_copy(k).start()
        return 0

    lax.fori_loop(0, groups, filtered, 0)

    def drain(k, _):
        s = lax.rem(gz + k, n)
        consts_copy(gz, s).wait_send()
        ph1_copy(gz, s).wait_send()
        ph2_copy(gz, s).wait_send()
        ct_copy(gz, s).wait_send()
        return 0

    lax.fori_loop(1, n, drain, 0)
    for k in range(others):
        cs_copy(k).wait_send()

    def drain_out(k, _):
        out_copy(k).wait()
        return 0

    lax.fori_loop(0, groups, drain_out, 0)


def local_step(sizes, density, design_mask, energy, decay, case_index, case_weight):
    n, ngx, ngy, lx, ly, lz, cells = sizes
    groups = lx // XG
    per = XG * ly
    others = ngx * ngy - 1
    dma = pltpu.SemaphoreType.DMA
    anywhere = pl.BlockSpec(memory_space=pl.ANY)
    smem = pl.BlockSpec(memory_space=pltpu.SMEM)
    return pl.pallas_call(
        functools.partial(kernel, sizes),
        out_shape=(
            jax.ShapeDtypeStruct((lx, ly, lz), F32),
            jax.ShapeDtypeStruct((CASES,), F32),
        ),
        in_specs=[anywhere, anywhere, anywhere, pl.BlockSpec(memory_space=pltpu.VMEM), smem, smem],
        out_specs=(anywhere, smem),
        scratch_shapes=[
            pltpu.VMEM((lx, ly, lz), F32),
            pltpu.VMEM((lx, ly, lz), jnp.int32),
            pltpu.VMEM((CASES, lx, ly, lz), BF16),
            pltpu.VMEM((lx, ly, lz), F32),
            pltpu.VMEM((per, 2 * CASES * lz), BF16),
            pltpu.VMEM((2 * CASES * lz, 2 * lz), BF16),
            pltpu.VMEM((16, 2 * CASES * lz), BF16),
            pltpu.VMEM((32, lz), BF16),
            pltpu.VMEM((lx + 2 * RADIUS, ly + 2 * YO, lz), F32),
            pltpu.VMEM((XG, ly + 2 * YO, lz), F32),
            pltpu.VMEM((lx, ly, lz), F32),
            pltpu.VMEM((16, lz), F32),
            pltpu.VMEM((n, 16, lz), F32),
            pltpu.VMEM((n, 8, lz), F32),
            pltpu.VMEM((n, 8, lz), F32),
            pltpu.VMEM((n, 8, lz), F32),
            pltpu.VMEM((n, 8, lz), F32),
            pltpu.VMEM((n, 8, lz), F32),
            pltpu.VMEM((8, lz), F32),
            pltpu.VMEM((others, 8, lz), F32),
            pltpu.VMEM((8, lz), F32),
            pltpu.VMEM((n, 8, lz), F32),
            pltpu.VMEM((RADIUS, ly, lz), BF16),
            pltpu.VMEM((RADIUS, ly, lz), BF16),
            pltpu.VMEM((2, RADIUS, lx, lz), BF16),
            pltpu.VMEM((2, RADIUS, lx, lz), BF16),
            pltpu.VMEM((2, RADIUS, RADIUS, lz), BF16),
            pltpu.VMEM((2, RADIUS, RADIUS, lz), BF16),
            dma((3, groups)),
            dma((groups,)),
            dma((n,)),
            dma((n,)),
            dma((n,)),
            dma((n,)),
            dma((n,)),
            dma((n,)),
            dma((others,)),
            dma((others,)),
            dma((n,)),
            dma((n,)),
            dma(()),
            dma(()),
            dma((2,)),
            dma((2,)),
            dma((2,)),
            dma((2,)),
        ],
        compiler_params=pltpu.CompilerParams(
            collective_id=0, has_side_effects=True, vmem_limit_bytes=56 * 1024 * 1024
        ),
        name="sensitivity",
    )(density, design_mask, energy, decay, case_index, case_weight)


def solution(mesh):
    shape = mesh.shape
    n, ngx, ngy = shape["gz"], shape["gx"], shape["gy"]

    def whole(density, design_mask, energy, decay, case_index, case_weight):
        nx, ny, nz = density.shape
        sizes = (n, ngx, ngy, nx // ngx, ny // ngy, nz // n, nx * ny * nz)
        return jax.shard_map(
            functools.partial(local_step, sizes),
            mesh=mesh,
            in_specs=(
                P("gx", "gy", "gz"), P("gx", "gy", "gz"), P(None, "gx", "gy", "gz"), P(None, "gz"), P(), P(),
            ),
            out_specs=(P("gx", "gy", "gz"), P()),
            check_vma=False,
        )(density, design_mask, energy, decay, case_index, case_weight)

    return whole
```

```python
import functools
import math

import jax
import jax.numpy as jnp
from jax import lax
from jax.experimental import pallas as pl
from jax.experimental.pallas import tpu as pltpu
from jax.sharding import PartitionSpec as P

CASES = 4
RADIUS = 3
F32 = jnp.float32
BF16 = jnp.bfloat16
MESH = pl.DeviceIdType.MESH
HIGH = lax.Precision.HIGHEST
XG = 8
BATCH = 2
EARLY = 4
YO = 8

_raw = [math.exp(-2.0 * k * k / (RADIUS * RADIUS)) for k in range(-RADIUS, RADIUS + 1)]
TAPS = [t / sum(_raw) for t in _raw]


def dot(a, b, ca, cb, precision=None):
    return lax.dot_general(a, b, (((ca,), (cb,)), ((), ())), precision=precision, preferred_element_type=F32)


def split(value):
    hi = value.astype(BF16)
    return hi, (value - hi.astype(F32)).astype(BF16)


def split_small(value):
    wide = value * 65537.0
    hi = wide - (wide - value)
    return hi.astype(BF16), (value - hi).astype(BF16)


def taps(get):
    acc = TAPS[RADIUS] * get(RADIUS)
    for t in range(RADIUS):
        acc = acc + TAPS[t] * (get(t) + get(2 * RADIUS - t))
    return acc


def kernel(
    sizes, dens_hbm, mask_hbm, en_hbm, decay_ref, index_ref, weight_ref,
    fm, scale, fc, vmap, comp_out,
    dens, mask, en, lhs, maps, coef, ext, tmp,
    consts_out, consts_in, fh_out, fh_in, fin, carry_out, cx, yf, yr,
    cs_out, cs_in, ct_out, ct_in, xs_out, xs_in, ys_out, ys_in, ds_out, ds_in, st_out, st_in, st_sum,
    load_sem, cst_s, cst_r, ph1_s, ph1_r, ph2_s, ph2_r, cs_s, cs_r, ct_s, ct_r,
    xs_s, xs_r, ys_s, ys_r, ds_s, ds_r, cb_s, cb_r, st_s, st_r, dg_s, dg_r,
):
    n, ngx, ngy, lx, ly, lz, cells = sizes
    groups = lx // XG
    per = XG * ly
    blocks = per // lz
    gz, gx, gy = lax.axis_index("gz"), lax.axis_index("gx"), lax.axis_index("gy")
    others = ngx * ngy - 1
    mine = gz // blocks

    def peer(k):
        flat = lax.rem(gx * ngy + gy + 1 + k, ngx * ngy)
        return {"gz": gz, "gx": flat // ngy, "gy": lax.rem(flat, ngy)}

    def group_at(i):
        j = (i + 1) // 2
        off = jnp.where(lax.rem(i, 2) == 1, groups // 2 - j, groups // 2 + j)
        return lax.rem(mine + off, groups)

    def each_far(body):
        for k in sorted(range(1, n), key=lambda k: -min(k // blocks, (n - k) // blocks)):
            body(jnp.where(gz + k >= n, gz + k - n, gz + k))

    def end(ref, sem):
        pltpu.make_async_copy(ref, ref, sem).wait()

    def loads(k):
        rows = pl.ds(k * XG, XG)
        return (
            pltpu.make_async_copy(dens_hbm.at[rows], dens.at[rows], load_sem.at[0, k]),
            pltpu.make_async_copy(mask_hbm.at[rows], mask.at[rows], load_sem.at[1, k]),
            pltpu.make_async_copy(en_hbm.at[:, rows], en.at[:, rows], load_sem.at[2, k]),
        )

    def start_loads(i, _):
        for copy in loads(group_at(i)):
            copy.start()
        return 0

    lax.fori_loop(0, groups, start_loads, 0)

    for i in (0, 1, n + 2, n + 3):
        cx[i] = jnp.zeros((8, lz), F32)
    st_in[...] = jnp.zeros_like(st_in)

    barrier = pltpu.get_barrier_semaphore()

    def greet(k, _):
        pl.semaphore_signal(barrier, inc=1, device_id={"gz": lax.rem(gz + k, n)}, device_id_type=MESH)
        return 0

    lax.fori_loop(1, n, greet, 0)
    for k in range(others):
        pl.semaphore_signal(barrier, inc=1, device_id=peer(k), device_id_type=MESH)

    decay = jnp.concatenate([decay_ref[...], decay_ref[...]], axis=0)
    logs = jnp.log(decay)
    row = lax.broadcasted_iota(jnp.int32, (lz, lz), 0)
    col = lax.broadcasted_iota(jnp.int32, (lz, lz), 1)
    low, high = row <= col, row >= col
    up = dot(logs, low.astype(F32), 1, 0, HIGH)
    down = dot(logs, high.astype(F32), 1, 0, HIGH)
    keep = 1.0 - decay
    columns = jnp.transpose(jnp.concatenate([up, down, keep, keep], axis=0))
    total = up[:, lz - 1 : lz]
    fwd_last = jnp.exp(total - up) * keep
    first = jnp.exp(down[:, 0:1] - down) * keep
    lead = jnp.exp(up)
    trail = jnp.exp(down)
    rows8 = lax.broadcasted_iota(jnp.int32, (8, lz), 0)
    rows16 = lax.broadcasted_iota(jnp.int32, (16, lz), 0)
    lane = lax.broadcasted_iota(jnp.int32, (8, lz), 1)
    couple = jnp.sum(first * lead, axis=1, keepdims=True)
    consts_out[...] = jnp.where(rows8 < CASES, jnp.exp(total), couple)
    consts_in[gz] = consts_out[...]

    vals = jnp.zeros((8, lz), F32)
    for c in range(CASES):
        wc = weight_ref[index_ref[c]] * -3.0
        up_col, down_col, keep_col = columns[:, c : c + 1], columns[:, 8 + c : 9 + c], columns[:, 16 + c : 17 + c]
        fwd_t = jnp.where(low, jnp.exp(jnp.where(low, up[c : c + 1] - up_col, 0.0)), 0.0) * keep_col
        bwd_t = jnp.where(high, jnp.exp(jnp.where(high, down[c : c + 1] - down_col, 0.0)), 0.0) * keep_col
        both = dot(fwd_t, bwd_t, 1, 0, HIGH) * wc
        hi, lo = split(both)
        for half in range(2):
            at = (2 * c + half) * lz
            maps[at : at + lz, 0:lz] = hi
            maps[at : at + lz, lz : 2 * lz] = lo
        hrow = dot(first, fwd_t, 1, 1, HIGH)
        lead_map = dot(lead, bwd_t, 1, 0, HIGH)
        cblock = jnp.where(rows8 == c, fwd_last, 0.0)
        cblock = jnp.where(rows8 == c + CASES, hrow, cblock)
        chi = cblock.astype(BF16).astype(F32)
        pair = jnp.concatenate([chi, cblock - chi], axis=0).astype(BF16)
        for half in range(2):
            at = (2 * c + half) * lz
            coef[0:16, at : at + lz] = pair
            coef[16:32, at : at + lz] = (rows16 == c).astype(F32).astype(BF16)
        vals = jnp.where(rows8 == c, lead_map * wc, vals)
        vals = jnp.where(rows8 == c + CASES, trail * wc, vals)
    vhi = vals.astype(BF16).astype(F32)
    vmap[...] = jnp.concatenate([vhi, vhi, vals - vhi, jnp.zeros((8, lz), F32)], axis=0).astype(BF16)

    def local(at, sums):
        k = group_at(at)
        for copy in loads(k):
            copy.wait()
        for i in range(XG):
            x = k * XG + i
            d, m = dens[x], mask[x]
            dense = jnp.where(m == 1, 0.001, jnp.where(m == 2, 1.0, d))
            cube = dense * dense * dense
            for c in range(CASES):
                hi, lo = split_small(cube * en[c, x].astype(F32))
                lhs[k, i * ly : (i + 1) * ly, 2 * c * lz : (2 * c + 1) * lz] = hi
                lhs[k, i * ly : (i + 1) * ly, (2 * c + 1) * lz : (2 * c + 2) * lz] = lo
        fh = dot(coef[...], lhs[k], 1, 1)
        for b in range(blocks):
            piece = fh[:, b * lz : (b + 1) * lz]
            fh_out[k * blocks + b] = piece[0:8] + piece[8:16]
            sums = sums + piece[16:24]
        return sums

    def to_slab(src, dst, send, recv, k):
        return pltpu.make_async_remote_copy(
            src_ref=src, dst_ref=dst, send_sem=send, recv_sem=recv,
            device_id={"gz": k}, device_id_type=MESH,
        )

    def consts_copy(src, dst):
        return to_slab(consts_out, consts_in.at[src], cst_s, cst_r, dst)

    def ph1_copy(src, dst):
        return to_slab(fh_out.at[dst], fh_in.at[src], ph1_s, ph1_r, dst)

    def ph2_copy(src, dst):
        return to_slab(carry_out.at[dst], cx.at[2 + src], ph2_s, ph2_r, dst)

    def ct_copy(src, dst):
        return to_slab(ct_out, ct_in.at[src], ct_s, ct_r, dst)

    def send_group(at):
        for b in range(blocks):
            p = group_at(at) * blocks + b

            @pl.when(p != gz)
            def _():
                ph1_copy(gz, p).start()

    sums = lax.fori_loop(0, EARLY, local, jnp.zeros((8, lz), F32))
    pl.semaphore_wait(barrier, n - 1 + others)
    for at in range(EARLY):
        send_group(at)
    each_far(lambda p: consts_copy(gz, p).start())

    def local_send(at, sums):
        sums = local(at, sums)
        send_group(at)
        return sums

    sums = lax.fori_loop(EARLY, groups, local_send, sums)
    fh_in[gz] = fh_out[gz]

    sums = jnp.sum(sums, axis=1, keepdims=True)
    part = jnp.sum(jnp.where(rows8 == lane, sums, 0.0), axis=0, keepdims=True)
    cs_out[...] = part

    def cs_copy(k):
        return pltpu.make_async_remote_copy(
            src_ref=cs_out, dst_ref=cs_in.at[k], send_sem=cs_s.at[k], recv_sem=cs_r.at[k],
            device_id=peer(k), device_id_type=MESH,
        )

    for k in range(others):
        cs_copy(k).start()

    for j in range(RADIUS):
        ext[j] = jnp.zeros((ly + 2 * YO, lz), F32)
        ext[RADIUS + lx + j] = jnp.zeros((ly + 2 * YO, lz), F32)
    ext[:, 0:YO] = jnp.zeros((lx + 2 * RADIUS, YO, lz), F32)
    ext[:, YO + ly :] = jnp.zeros((lx + 2 * RADIUS, YO, lz), F32)

    def smoothed(k, _):
        full = dot(lhs[k], maps[...], 1, 0)
        full = full[:, :lz] + full[:, lz:]
        ext[pl.ds(RADIUS + k * XG, XG), YO : YO + ly, :] = full.reshape(XG, ly, lz)
        for i in range(XG):
            x = k * XG + i
            scale[x] = jnp.where(mask[x] == 0, 1.0 / jnp.maximum(dens[x], 0.1), 0.0)
        return 0

    lax.fori_loop(0, groups, smoothed, 0)

    xs_at = jnp.where(gx == 0, lx - RADIUS, 0)
    for j in range(RADIUS):
        xs_out[j] = ext[RADIUS + xs_at + j, YO : YO + ly, :].astype(BF16)
    for side in range(2):
        for j in range(RADIUS):
            y = YO + (j if side == 0 else ly - RADIUS + j)
            ys_out[side, j] = ext[RADIUS : RADIUS + lx, y, :].astype(BF16)
            ds_out[side, j] = ext[pl.ds(RADIUS + xs_at, RADIUS), y, :].astype(BF16)

    def beside(src, dst, send, recv, where):
        return pltpu.make_async_remote_copy(
            src_ref=src, dst_ref=dst, send_sem=send, recv_sem=recv, device_id=where, device_id_type=MESH
        )

    def x_copy():
        return beside(xs_out, xs_in, xs_s, xs_r, {"gx": 1 - gx})

    def y_copy(side, to):
        return beside(ys_out.at[side], ys_in.at[1 - side], ys_s.at[side], ys_r.at[1 - side], {"gy": to})

    def d_copy(side, to):
        where = {"gx": 1 - gx, "gy": to}
        return beside(ds_out.at[side], ds_in.at[1 - side], ds_s.at[side], ds_r.at[1 - side], where)

    def blocks_copy():
        src = jnp.where(gx == 0, n, 2)
        dst = jnp.where(gx == 0, 0, n + 2)
        return beside(cx.at[pl.ds(src, 2)], cx.at[pl.ds(dst, 2)], cb_s, cb_r, {"gx": 1 - gx})

    def blocks_arrive():
        dst = jnp.where(gx == 0, n + 2, 0)
        return beside(cx.at[pl.ds(dst, 2)], cx.at[pl.ds(dst, 2)], cb_s, cb_r, {"gx": 1 - gx})

    def strip_copy(side, to):
        where = {"gy": to}
        return beside(st_out.at[side], st_in.at[1 - side, 1:3], st_s.at[side], st_r.at[1 - side], where)

    def corner_copy(side, to):
        where = {"gx": 1 - gx, "gy": to}
        dst = st_in.at[1 - side, jnp.where(gx == 0, 0, 3)]
        return beside(st_out.at[side, 1 - gx], dst, dg_s.at[side], dg_r.at[1 - side], where)

    def corner_arrive(side, to):
        where = {"gx": 1 - gx, "gy": to}
        dst = st_in.at[side, jnp.where(gx == 0, 3, 0)]
        return beside(st_out.at[side, 1 - gx], dst, dg_s.at[side], dg_r.at[side], where)

    def sides(body):
        @pl.when(gy > 0)
        def _():
            body(0, gy - 1)

        @pl.when(gy < ngy - 1)
        def _():
            body(1, gy + 1)

    x_copy().start()

    def send_halo(side, to):
        y_copy(side, to).start()
        d_copy(side, to).start()

    sides(send_halo)

    def gains(s):
        both = consts_in[s]
        turned = pltpu.roll(both, CASES, 0)
        return jnp.where(rows8 < CASES, both, turned), jnp.where(rows8 < CASES, turned, both)

    def ascend(s, state):
        fin[s] = state
        return gains(s)[0] * state + fh_in[s]

    end(fh_in.at[0 : n - 1], cst_r)
    end(fh_in.at[0 : n - 1], ph1_r)
    lax.fori_loop(0, n, ascend, jnp.zeros((8, lz), F32))

    def descend(k, state):
        s = n - 1 - k
        entering = fin[s]
        carry_out[s] = jnp.where(rows8 < CASES, entering, state)
        gain, mix = gains(s)
        return gain * state + fh_in[s] + mix * pltpu.roll(entering, CASES, 0)

    lax.fori_loop(0, n, descend, jnp.zeros((8, lz), F32))
    each_far(lambda p: ph2_copy(gz, p).start())
    cx[2 + gz] = carry_out[gz]
    for k in range(others):
        cs_copy(k).wait_recv()
        part = part + cs_in[k]
    ct_out[...] = part
    ct_in[gz] = part
    each_far(lambda p: ct_copy(gz, p).start())


    halo_x = jnp.where(gx == 0, RADIUS + lx, 0)
    x_copy().wait()
    ext[pl.ds(halo_x, RADIUS), YO : YO + ly, :] = xs_in[...].astype(F32)

    def take(side, to):
        for copy in (y_copy, d_copy):
            copy(side, to).wait_send()
            copy(1 - side, to).wait_recv()
        for j in range(RADIUS):
            y = YO + (j - RADIUS if side == 0 else ly + j)
            ext[RADIUS : RADIUS + lx, y, :] = ys_in[side, j].astype(F32)
            ext[pl.ds(halo_x, RADIUS), y, :] = ds_in[side, j].astype(F32)

    sides(take)

    def filtered(k, _):
        for i in range(XG):
            x = k * XG + i
            tmp[i] = taps(lambda t: ext[x + t])
            fm[x] = taps(lambda t: tmp[i, YO - RADIUS + t : YO - RADIUS + t + ly, :])
        return 0

    lax.fori_loop(0, groups, filtered, 0)

    end(fh_in.at[0 : n - 1], ph2_r)
    blocks_copy().start()
    half_y = lax.rem(lane, ly)
    slot = half_y // 4
    for side in range(2):
        y0 = 0 if side == 0 else ly - RADIUS
        for half in range(2):
            packed = jnp.zeros((8, lz), F32)
            for q in range(n // 2):
                moved = pltpu.roll(cx[2 + half * (n // 2) + q], (4 * q - y0) % lz, 1)
                packed = jnp.where(slot == q, moved, packed)
            st_out[side, half] = packed

    def send_strip(side, to):
        strip_copy(side, to).start()
        corner_copy(side, to).start()

    sides(send_strip)
    def add_ct(s, state):
        return state + ct_in[s]

    end(ct_in.at[0 : n - 1], ct_r)
    comp_out[...] = lax.fori_loop(0, n, add_ct, jnp.zeros((1, lz), F32)) * (1.0 / cells)

    for sem in (cst_s, ph1_s, ph2_s):
        end(fh_in.at[0 : n - 1], sem)
    end(ct_in.at[0 : n - 1], ct_s)
    for k in range(others):
        cs_copy(k).wait_send()

    def along_y(k, _):
        for b in range(4):
            i = k * 4 + b
            state = cx[2 + i]
            acc = TAPS[RADIUS] * state
            for t in range(1, RADIUS + 1):
                down_y = jnp.where(half_y >= t, pltpu.roll(state, t, 1), 0.0)
                up_y = jnp.where(half_y < ly - t, pltpu.roll(state, lz - t, 1), 0.0)
                acc = acc + TAPS[RADIUS + t] * (down_y + up_y)
            yf[2 + i] = acc
        return 0

    lax.fori_loop(0, n // 4, along_y, 0)

    blocks_copy().wait_send()
    blocks_arrive().wait_recv()
    for i in (0, 1, n + 2, n + 3):
        state = cx[i]
        acc = TAPS[RADIUS] * state
        for t in range(1, RADIUS + 1):
            down_y = jnp.where(half_y >= t, pltpu.roll(state, t, 1), 0.0)
            up_y = jnp.where(half_y < ly - t, pltpu.roll(state, lz - t, 1), 0.0)
            acc = acc + TAPS[RADIUS + t] * (down_y + up_y)
        yf[i] = acc

    def take_strip(side, to):
        strip_copy(side, to).wait_send()
        corner_copy(side, to).wait_send()
        strip_copy(1 - side, to).wait_recv()
        corner_arrive(side, to).wait_recv()

    sides(take_strip)

    for side in range(2):
        for quarter in range(4):
            strip = st_in[side, quarter]
            total_y = jnp.zeros((8, lz), F32)
            for y in range(RADIUS):
                for j in range(RADIUS):
                    far = y + j + 1
                    if far > RADIUS:
                        continue
                    at = RADIUS - 1 - j if side == 0 else j
                    to = y if side == 0 else RADIUS - 1 - y
                    moved = strip if at == to else pltpu.roll(strip, (to - at) % lz, 1)
                    total_y = total_y + jnp.where(lax.rem(lane, 4) == to, TAPS[RADIUS + far] * moved, 0.0)
            st_sum[side, quarter] = total_y

    def add_strips(k, _):
        for b in range(4):
            i = k * 4 + b
            at = i + n // 2 - 2
            quarter, q = at // (n // 2), lax.rem(at, n // 2)
            mine_y = slot == q
            low_y = pltpu.roll(jnp.where(mine_y, st_sum[0, quarter], 0.0), lz - 4 * q, 1)
            high_y = pltpu.roll(jnp.where(mine_y, st_sum[1, quarter], 0.0), lz + ly - RADIUS - 4 * q, 1)
            acc = yf[i] + low_y + high_y
            yf[i] = acc
            yr[i] = pltpu.roll(acc, ly, 1)
        return 0

    lax.fori_loop(0, (n + 4) // 4, add_strips, 0)
    first_half = lane < ly

    def along_x(k, _):
        for b in range(4):
            p = k * 4 + b
            i = p + 2
            near = yr[i] + jnp.where(first_half, yr[i - 1], yr[i + 1])
            far = jnp.where(first_half, yr[i - 2] + yr[i + 1], yr[i - 1] + yr[i + 2])
            acc = TAPS[RADIUS] * yf[i] + TAPS[RADIUS + 1] * near
            fc[p] = acc + TAPS[RADIUS + 2] * (yf[i - 1] + yf[i + 1]) + TAPS[RADIUS + 3] * far
        return 0

    lax.fori_loop(0, n // 4, along_x, 0)


def last(fm, scale, fc, vmap, comp_in, out_hbm, comp_out, out, sem):
    lx, ly, lz = fm.shape
    rows_per = lz // ly
    n = fc.shape[0]
    step = 4
    for c in range(CASES):
        comp_out[c] = jnp.sum(comp_in[0:1, c : c + 1])

    def out_copy(k):
        rows = pl.ds(k * step * rows_per, step * rows_per)
        return pltpu.make_async_copy(out.at[rows], out_hbm.at[rows], sem.at[k])

    def finish(t, _):
        for b in range(BATCH * step):
            p = t * BATCH * step + b
            state = fc[p]
            hi = state.astype(BF16).astype(F32)
            stack = jnp.concatenate([hi, state - hi, hi, jnp.zeros((8, lz), F32)], axis=0)
            add = dot(jnp.transpose(stack).astype(BF16), vmap[...], 1, 0).reshape(rows_per, ly, lz)
            at = pl.ds(p * rows_per, rows_per)
            out[at] = (fm[at] + add) * scale[at]
        for b in range(BATCH):
            out_copy(t * BATCH + b).start()
        return 0

    lax.fori_loop(0, n // (BATCH * step), finish, 0)

    def drain_out(k, _):
        out_copy(k).wait()
        return 0

    lax.fori_loop(0, n // step, drain_out, 0)


def local_step(sizes, density, design_mask, energy, decay, case_index, case_weight):
    n, ngx, ngy, lx, ly, lz, cells = sizes
    groups = lx // XG
    per = XG * ly
    others = ngx * ngy - 1
    dma = pltpu.SemaphoreType.DMA
    anywhere = pl.BlockSpec(memory_space=pltpu.HBM)
    smem = pl.BlockSpec(memory_space=pltpu.SMEM)
    vmem = pl.BlockSpec(memory_space=pltpu.VMEM)
    state = pltpu.VMEM((n, 8, lz), F32)
    fm, scale, fc, vmap, comp = pl.pallas_call(
        functools.partial(kernel, sizes),
        out_shape=(
            jax.ShapeDtypeStruct((lx, ly, lz), F32),
            jax.ShapeDtypeStruct((lx, ly, lz), F32),
            jax.ShapeDtypeStruct((n, 8, lz), F32),
            jax.ShapeDtypeStruct((32, lz), BF16),
            jax.ShapeDtypeStruct((1, lz), F32),
        ),
        in_specs=[anywhere, anywhere, anywhere, vmem, smem, smem],
        out_specs=(vmem,) * 5,
        scratch_shapes=[
            pltpu.VMEM((lx, ly, lz), F32),
            pltpu.VMEM((lx, ly, lz), jnp.int32),
            pltpu.VMEM((CASES, lx, ly, lz), BF16),
            pltpu.VMEM((groups, per, 2 * CASES * lz), BF16),
            pltpu.VMEM((2 * CASES * lz, 2 * lz), BF16),
            pltpu.VMEM((32, 2 * CASES * lz), BF16),
            pltpu.VMEM((lx + 2 * RADIUS, ly + 2 * YO, lz), F32),
            pltpu.VMEM((XG, ly + 2 * YO, lz), F32),
            pltpu.VMEM((8, lz), F32),
            state,
            state,
            state,
            state,
            state,
            pltpu.VMEM((n + 4, 8, lz), F32),
            pltpu.VMEM((n + 4, 8, lz), F32),
            pltpu.VMEM((n + 4, 8, lz), F32),
            pltpu.VMEM((1, lz), F32),
            pltpu.VMEM((others, 1, lz), F32),
            pltpu.VMEM((1, lz), F32),
            pltpu.VMEM((n, 1, lz), F32),
            pltpu.VMEM((RADIUS, ly, lz), BF16),
            pltpu.VMEM((RADIUS, ly, lz), BF16),
            pltpu.VMEM((2, RADIUS, lx, lz), BF16),
            pltpu.VMEM((2, RADIUS, lx, lz), BF16),
            pltpu.VMEM((2, RADIUS, RADIUS, lz), BF16),
            pltpu.VMEM((2, RADIUS, RADIUS, lz), BF16),
            pltpu.VMEM((2, 2, 8, lz), F32),
            pltpu.VMEM((2, 4, 8, lz), F32),
            pltpu.VMEM((2, 4, 8, lz), F32),
            dma((3, groups)),
            dma(()),
            dma(()),
            dma(()),
            dma(()),
            dma(()),
            dma(()),
            dma((others,)),
            dma((others,)),
            dma(()),
            dma(()),
            dma(()),
            dma(()),
            dma((2,)),
            dma((2,)),
            dma((2,)),
            dma((2,)),
            dma(()),
            dma(()),
            dma((2,)),
            dma((2,)),
            dma((2,)),
            dma((2,)),
        ],
        compiler_params=pltpu.CompilerParams(
            collective_id=0, has_side_effects=True, vmem_limit_bytes=40 * 1024 * 1024
        ),
        name="states",
    )(*(pltpu.with_memory_space_constraint(v, pltpu.HBM) for v in (density, design_mask, energy, decay, case_index, case_weight)))
    return pl.pallas_call(
        last,
        out_shape=(
            jax.ShapeDtypeStruct((lx, ly, lz), F32),
            jax.ShapeDtypeStruct((CASES,), F32),
        ),
        in_specs=[vmem] * 5,
        out_specs=(anywhere, smem),
        scratch_shapes=[pltpu.VMEM((lx, ly, lz), F32), dma((n // 4,))],
        compiler_params=pltpu.CompilerParams(vmem_limit_bytes=20 * 1024 * 1024),
        name="result",
    )(fm, scale, fc, vmap, comp)


def solution(mesh):
    shape = mesh.shape
    n, ngx, ngy = shape["gz"], shape["gx"], shape["gy"]

    def whole(density, design_mask, energy, decay, case_index, case_weight):
        nx, ny, nz = density.shape
        sizes = (n, ngx, ngy, nx // ngx, ny // ngy, nz // n, nx * ny * nz)
        return jax.shard_map(
            functools.partial(local_step, sizes),
            mesh=mesh,
            in_specs=(
                P("gx", "gy", "gz"), P("gx", "gy", "gz"), P(None, "gx", "gy", "gz"), P(None, "gz"), P(), P(),
            ),
            out_specs=(P("gx", "gy", "gz"), P()),
            check_vma=False,
        )(density, design_mask, energy, decay, case_index, case_weight)

    return whole
```

```python
import functools
import math

import jax
import jax.numpy as jnp
from jax import lax
from jax.experimental import pallas as pl
from jax.experimental.pallas import tpu as pltpu
from jax.sharding import PartitionSpec as P

CASES = 4
RADIUS = 3
F32 = jnp.float32
BF16 = jnp.bfloat16
MESH = pl.DeviceIdType.MESH
HIGH = lax.Precision.HIGHEST
XG = 8
BATCH = 8
PIECES = 8
EARLY = 4
YO = 8

_raw = [math.exp(-2.0 * k * k / (RADIUS * RADIUS)) for k in range(-RADIUS, RADIUS + 1)]
TAPS = [t / sum(_raw) for t in _raw]


def dot(a, b, ca, cb, precision=None):
    return lax.dot_general(a, b, (((ca,), (cb,)), ((), ())), precision=precision, preferred_element_type=F32)


def split(value):
    hi = value.astype(BF16)
    return hi, (value - hi.astype(F32)).astype(BF16)


def taps(get):
    acc = TAPS[RADIUS] * get(RADIUS)
    for t in range(RADIUS):
        acc = acc + TAPS[t] * (get(t) + get(2 * RADIUS - t))
    return acc


def kernel(
    sizes, dens_hbm, mask_hbm, en_hbm, decay_ref, index_ref, weight_ref,
    fm, comp_out,
    dens, mask, en, fwd, lhs, maps, coef, ext, tmp, scale, fc, vmap, inv, cf,
    consts_out, consts_in, gain, mix, fh_out, fh_in, fin, carry_out, cx, yf, yr,
    cs_out, cs_in, ct_out, ct_in, xs_out, xs_in, ys_out, ys_in, ds_out, ds_in, st_out, st_in, st_sum,
    load_sem, cst_s, cst_r, ph1_s, ph1_r, ph2_s, ph2_r, cs_s, cs_r, ct_s, ct_r,
    xs_s, xs_r, ys_s, ys_r, ds_s, ds_r, cb_s, cb_r, st_s, st_r, dg_s, dg_r,
):
    n, ngx, ngy, lx, ly, lz, cells = sizes
    groups = lx // XG
    per = XG * ly
    blocks = per // lz
    gz, gx, gy = lax.axis_index("gz"), lax.axis_index("gx"), lax.axis_index("gy")
    others = ngx * ngy - 1
    mine = gz // blocks

    def peer(k):
        flat = lax.rem(gx * ngy + gy + 1 + k, ngx * ngy)
        return {"gz": gz, "gx": flat // ngy, "gy": lax.rem(flat, ngy)}

    def group_at(i):
        j = (i + 1) // 2
        off = jnp.where(lax.rem(i, 2) == 1, groups // 2 - j, groups // 2 + j)
        return lax.rem(mine + off, groups)

    def each_far(body):
        for k in sorted(range(1, n), key=lambda k: -min(k // blocks, (n - k) // blocks)):
            body(jnp.where(gz + k >= n, gz + k - n, gz + k))

    def end(ref, sem):
        pltpu.make_async_copy(ref, ref, sem).wait()

    for i in (0, 1, n + 2, n + 3):
        cx[i] = jnp.zeros((8, lz), BF16)
    st_in[...] = jnp.zeros_like(st_in)

    def loads(k):
        rows = pl.ds(k * XG, XG)
        return (
            pltpu.make_async_copy(dens_hbm.at[rows], dens.at[rows], load_sem.at[0, k]),
            pltpu.make_async_copy(mask_hbm.at[rows], mask.at[rows], load_sem.at[1, k]),
            pltpu.make_async_copy(en_hbm.at[:, rows], en.at[:, rows], load_sem.at[2, k]),
        )

    def start_loads(i, _):
        for copy in loads(group_at(i)):
            copy.start()
        return 0

    lax.fori_loop(0, 2, start_loads, 0)
    barrier = pltpu.get_barrier_semaphore()
    each_far(lambda p: pl.semaphore_signal(barrier, inc=1, device_id={"gz": p}, device_id_type=MESH))
    for k in range(others):
        pl.semaphore_signal(barrier, inc=1, device_id=peer(k), device_id_type=MESH)
    lax.fori_loop(2, groups, start_loads, 0)

    decay = jnp.concatenate([decay_ref[...], decay_ref[...]], axis=0)
    logs = jnp.log(decay)
    row = lax.broadcasted_iota(jnp.int32, (lz, lz), 0)
    col = lax.broadcasted_iota(jnp.int32, (lz, lz), 1)
    low, high = row <= col, row >= col
    up = dot(logs, low.astype(F32), 1, 0, HIGH)
    down = dot(logs, high.astype(F32), 1, 0, HIGH)
    keep = 1.0 - decay
    columns = jnp.transpose(jnp.concatenate([up, down, keep, keep], axis=0))
    total = up[:, lz - 1 : lz]
    fwd_last = jnp.exp(total - up) * keep
    first = jnp.exp(down[:, 0:1] - down) * keep
    lead = jnp.exp(up)
    trail = jnp.exp(down)
    rows8 = lax.broadcasted_iota(jnp.int32, (8, lz), 0)
    rows16 = lax.broadcasted_iota(jnp.int32, (16, lz), 0)
    lane = lax.broadcasted_iota(jnp.int32, (8, lz), 1)
    couple = jnp.sum(first * lead, axis=1, keepdims=True)
    across = jnp.where(rows8 == lane, jnp.exp(total), jnp.where(rows8 + 8 == lane, couple, 0.0))
    consts_out[...] = jnp.sum(across, axis=0, keepdims=True)
    consts_in[gz] = consts_out[...]

    for c in range(CASES):
        fwd_t = jnp.where(low, jnp.exp(jnp.where(low, up[c : c + 1] - columns[:, c : c + 1], 0.0)), 0.0)
        fwd_t = fwd_t * columns[:, 16 + c : 17 + c]
        fwd[c] = fwd_t
        hrow = dot(first, fwd_t, 1, 1, HIGH)
        cblock = jnp.where(rows8 == c, fwd_last, 0.0)
        cblock = jnp.where(rows8 == c + CASES, hrow, cblock)
        chi = cblock.astype(BF16).astype(F32)
        pair = jnp.concatenate([chi, cblock - chi], axis=0).astype(BF16)
        for half in range(2):
            at = (2 * c + half) * lz
            coef[0:16, at : at + lz] = pair
            coef[16:32, at : at + lz] = (rows16 == c).astype(F32).astype(BF16)

    spots = lane.astype(F32) * 0.6180339887 + rows8.astype(F32) * 0.3247179572

    def stretch(p):
        phase = spots + jnp.asarray(p, jnp.int32).astype(F32) * 0.7548776662
        return 1.0 + (phase - jnp.floor(phase))

    def operand(k):
        return jnp.concatenate([lhs[k, c] for c in range(2 * CASES)], axis=1)

    def local(at, sums):
        k = group_at(at)
        for copy in loads(k):
            copy.wait()
        for i in range(XG):
            x = k * XG + i
            d, m = dens[x], mask[x]
            dense = jnp.where(m == 1, 0.001, jnp.where(m == 2, 1.0, d))
            cube = dense * dense * dense
            for c in range(CASES):
                hi, lo = split(cube * en[c, x].astype(F32))
                lhs[k, 2 * c, i * ly : (i + 1) * ly] = hi
                lhs[k, 2 * c + 1, i * ly : (i + 1) * ly] = lo
        fh = dot(coef[...], operand(k), 1, 1)
        for b in range(blocks):
            piece = fh[:, b * lz : (b + 1) * lz]
            fh_out[k * blocks + b] = ((piece[0:8] + piece[8:16]) * stretch(k * blocks + b)).astype(BF16)
            sums = sums + piece[16:24]
        return sums

    def to_slab(src, dst, send, recv, k):
        return pltpu.make_async_remote_copy(
            src_ref=src, dst_ref=dst, send_sem=send, recv_sem=recv,
            device_id={"gz": k}, device_id_type=MESH,
        )

    def consts_copy(src, dst):
        return to_slab(consts_out, consts_in.at[src], cst_s, cst_r, dst)

    def ph1_copy(src, dst):
        return to_slab(fh_out.at[dst], fh_in.at[src], ph1_s, ph1_r, dst)

    def ph2_copy(src, dst):
        return to_slab(carry_out.at[dst], cx.at[2 + src], ph2_s, ph2_r, dst)

    def ct_copy(src, dst):
        return to_slab(ct_out, ct_in.at[src], ct_s, ct_r, dst)

    def send_group(at):
        for b in range(blocks):
            p = group_at(at) * blocks + b

            @pl.when(p != gz)
            def _():
                ph1_copy(gz, p).start()

    sums = lax.fori_loop(0, EARLY, local, jnp.zeros((8, lz), F32))
    pl.semaphore_wait(barrier, n - 1 + others)
    for at in range(EARLY):
        send_group(at)
    each_far(lambda p: consts_copy(gz, p).start())

    def local_send(at, sums):
        sums = local(at, sums)
        send_group(at)
        return sums

    sums = lax.fori_loop(EARLY, groups, local_send, sums)
    fh_in[gz] = fh_out[gz]

    sums = jnp.sum(sums, axis=1, keepdims=True)
    part = jnp.sum(jnp.where(rows8 == lane, sums, 0.0), axis=0, keepdims=True)
    cs_out[...] = part

    def cs_copy(k):
        return pltpu.make_async_remote_copy(
            src_ref=cs_out, dst_ref=cs_in.at[k], send_sem=cs_s.at[k], recv_sem=cs_r.at[k],
            device_id=peer(k), device_id_type=MESH,
        )

    for k in range(others):
        cs_copy(k).start()

    vals = jnp.zeros((8, lz), F32)
    for c in range(CASES):
        wc = weight_ref[index_ref[c]] * -3.0
        bwd_t = jnp.where(high, jnp.exp(jnp.where(high, down[c : c + 1] - columns[:, 8 + c : 9 + c], 0.0)), 0.0)
        bwd_t = bwd_t * columns[:, 16 + c : 17 + c]
        hi, lo = split(dot(fwd[c], bwd_t, 1, 0, HIGH) * wc)
        for half in range(2):
            at = (2 * c + half) * lz
            maps[at : at + lz, 0:lz] = hi
            maps[at : at + lz, lz : 2 * lz] = lo
        lead_map = dot(lead, bwd_t, 1, 0, HIGH)
        vals = jnp.where(rows8 == c, lead_map * wc, vals)
        vals = jnp.where(rows8 == c + CASES, trail * wc, vals)
    vhi = vals.astype(BF16).astype(F32)
    vmap[...] = jnp.concatenate([vhi, vhi, vals - vhi, jnp.zeros((8, lz), F32)], axis=0).astype(BF16)

    for j in range(RADIUS):
        ext[j] = jnp.zeros((ly + 2 * YO, lz), F32)
        ext[RADIUS + lx + j] = jnp.zeros((ly + 2 * YO, lz), F32)
    ext[:, 0:YO] = jnp.zeros((lx + 2 * RADIUS, YO, lz), F32)
    ext[:, YO + ly :] = jnp.zeros((lx + 2 * RADIUS, YO, lz), F32)

    def smoothed(k, _):
        full = dot(operand(k), maps[...], 1, 0)
        full = full[:, :lz] + full[:, lz:]
        ext[pl.ds(RADIUS + k * XG, XG), YO : YO + ly, :] = full.reshape(XG, ly, lz)
        for i in range(XG):
            x = k * XG + i
            scale[x] = jnp.where(mask[x] == 0, 1.0 / jnp.maximum(dens[x], 0.1), 0.0)
        return 0

    lax.fori_loop(0, groups, smoothed, 0)

    xs_at = jnp.where(gx == 0, lx - RADIUS, 0)
    for j in range(RADIUS):
        xs_out[j] = ext[RADIUS + xs_at + j, YO : YO + ly, :].astype(BF16)
    for side in range(2):
        for j in range(RADIUS):
            y = YO + (j if side == 0 else ly - RADIUS + j)
            ys_out[side, j] = ext[RADIUS : RADIUS + lx, y, :].astype(BF16)
            ds_out[side, j] = ext[pl.ds(RADIUS + xs_at, RADIUS), y, :].astype(BF16)

    def beside(src, dst, send, recv, where):
        return pltpu.make_async_remote_copy(
            src_ref=src, dst_ref=dst, send_sem=send, recv_sem=recv, device_id=where, device_id_type=MESH
        )

    def x_copy():
        return beside(xs_out, xs_in, xs_s, xs_r, {"gx": 1 - gx})

    def y_copy(side, to):
        return beside(ys_out.at[side], ys_in.at[1 - side], ys_s.at[side], ys_r.at[1 - side], {"gy": to})

    def d_copy(side, to):
        where = {"gx": 1 - gx, "gy": to}
        return beside(ds_out.at[side], ds_in.at[1 - side], ds_s.at[side], ds_r.at[1 - side], where)

    def blocks_copy():
        src = jnp.where(gx == 0, n, 2)
        dst = jnp.where(gx == 0, 0, n + 2)
        return beside(cx.at[pl.ds(src, 2)], cx.at[pl.ds(dst, 2)], cb_s, cb_r, {"gx": 1 - gx})

    def blocks_arrive():
        dst = jnp.where(gx == 0, n + 2, 0)
        return beside(cx.at[pl.ds(dst, 2)], cx.at[pl.ds(dst, 2)], cb_s, cb_r, {"gx": 1 - gx})

    def strip_copy(side, to):
        where = {"gy": to}
        return beside(st_out.at[side], st_in.at[1 - side, 1:3], st_s.at[side], st_r.at[1 - side], where)

    def corner_copy(side, to):
        where = {"gx": 1 - gx, "gy": to}
        dst = st_in.at[1 - side, jnp.where(gx == 0, 0, 3)]
        return beside(st_out.at[side, 1 - gx], dst, dg_s.at[side], dg_r.at[1 - side], where)

    def corner_arrive(side, to):
        where = {"gx": 1 - gx, "gy": to}
        dst = st_in.at[side, jnp.where(gx == 0, 3, 0)]
        return beside(st_out.at[side, 1 - gx], dst, dg_s.at[side], dg_r.at[side], where)

    def sides(body):
        @pl.when(gy > 0)
        def _():
            body(0, gy - 1)

        @pl.when(gy < ngy - 1)
        def _():
            body(1, gy + 1)

    x_copy().start()

    def send_halo(side, to):
        y_copy(side, to).start()
        d_copy(side, to).start()

    sides(send_halo)

    for p in range(n):
        inv[p] = 1.0 / stretch(p)
    end(ct_in.at[0 : n - 1], cst_r)
    spread = jnp.transpose(jnp.concatenate([consts_in[s] for s in range(n)], axis=0))
    for s in range(n):
        gain[s] = jnp.broadcast_to(spread[0:8, s : s + 1], (8, lz))
        mix[s] = jnp.broadcast_to(spread[8:16, s : s + 1], (8, lz))
    end(fh_in.at[0 : n - 1], ph1_r)
    shrink, widen = 1.0 / stretch(gz), stretch(gz)
    state = jnp.zeros((8, lz), F32)
    for s in range(n):
        fin[s] = state
        state = gain[s] * state + fh_in[s].astype(F32) * shrink
    state = jnp.zeros((8, lz), F32)
    for s in reversed(range(n)):
        entering = fin[s]
        carry_out[s] = (jnp.where(rows8 < CASES, entering, state) * widen).astype(BF16)
        state = gain[s] * state + (fh_in[s].astype(F32) * shrink + mix[s] * pltpu.roll(entering, CASES, 0))
    each_far(lambda p: ph2_copy(gz, p).start())
    cx[2 + gz] = carry_out[gz]
    for k in range(others):
        cs_copy(k).wait_recv()
        part = part + cs_in[k]
    ct_out[...] = part
    ct_in[gz] = part
    each_far(lambda p: ct_copy(gz, p).start())


    halo_x = jnp.where(gx == 0, RADIUS + lx, 0)
    x_copy().wait()
    ext[pl.ds(halo_x, RADIUS), YO : YO + ly, :] = xs_in[...].astype(F32)

    def take(side, to):
        for copy in (y_copy, d_copy):
            copy(side, to).wait_send()
            copy(1 - side, to).wait_recv()
        for j in range(RADIUS):
            y = YO + (j - RADIUS if side == 0 else ly + j)
            ext[RADIUS : RADIUS + lx, y, :] = ys_in[side, j].astype(F32)
            ext[pl.ds(halo_x, RADIUS), y, :] = ds_in[side, j].astype(F32)

    sides(take)

    def filtered(k, _):
        for i in range(XG):
            x = k * XG + i
            tmp[i] = taps(lambda t: ext[x + t])
            fm[x] = taps(lambda t: tmp[i, YO - RADIUS + t : YO - RADIUS + t + ly, :])
        return 0

    lax.fori_loop(0, groups, filtered, 0)

    end(fh_in.at[0 : n - 1], ph2_r)
    blocks_copy().start()
    for p in range(n):
        cf[2 + p] = cx[2 + p].astype(F32) * inv[p]
    half_y = lax.rem(lane, ly)
    slot = half_y // 4
    for side in range(2):
        y0 = 0 if side == 0 else ly - RADIUS
        for half in range(2):
            packed = jnp.zeros((8, lz), F32)
            for q in range(n // 2):
                moved = pltpu.roll(cf[2 + half * (n // 2) + q], (4 * q - y0) % lz, 1)
                packed = jnp.where(slot == q, moved, packed)
            st_out[side, half] = packed

    def send_strip(side, to):
        strip_copy(side, to).start()
        corner_copy(side, to).start()

    sides(send_strip)
    def add_ct(s, state):
        return state + ct_in[s]

    end(ct_in.at[0 : n - 1], ct_r)
    comp_out[...] = lax.fori_loop(0, n, add_ct, jnp.zeros((1, lz), F32)) * (1.0 / cells)

    for sem in (ph1_s, ph2_s):
        end(fh_in.at[0 : n - 1], sem)
    for sem in (cst_s, ct_s):
        end(ct_in.at[0 : n - 1], sem)
    for k in range(others):
        cs_copy(k).wait_send()

    def along_y(k, _):
        for b in range(4):
            i = k * 4 + b
            state = cf[2 + i]
            acc = TAPS[RADIUS] * state
            for t in range(1, RADIUS + 1):
                down_y = jnp.where(half_y >= t, pltpu.roll(state, t, 1), 0.0)
                up_y = jnp.where(half_y < ly - t, pltpu.roll(state, lz - t, 1), 0.0)
                acc = acc + TAPS[RADIUS + t] * (down_y + up_y)
            yf[2 + i] = acc
        return 0

    lax.fori_loop(0, n // 4, along_y, 0)

    blocks_copy().wait_send()
    blocks_arrive().wait_recv()
    for i in (0, 1, n + 2, n + 3):
        state = cx[i].astype(F32) * inv[(i - 2) % n]
        acc = TAPS[RADIUS] * state
        for t in range(1, RADIUS + 1):
            down_y = jnp.where(half_y >= t, pltpu.roll(state, t, 1), 0.0)
            up_y = jnp.where(half_y < ly - t, pltpu.roll(state, lz - t, 1), 0.0)
            acc = acc + TAPS[RADIUS + t] * (down_y + up_y)
        yf[i] = acc

    def take_strip(side, to):
        strip_copy(side, to).wait_send()
        corner_copy(side, to).wait_send()
        strip_copy(1 - side, to).wait_recv()
        corner_arrive(side, to).wait_recv()

    sides(take_strip)

    for side in range(2):
        for quarter in range(4):
            strip = st_in[side, quarter]
            total_y = jnp.zeros((8, lz), F32)
            for y in range(RADIUS):
                for j in range(RADIUS):
                    far = y + j + 1
                    if far > RADIUS:
                        continue
                    at = RADIUS - 1 - j if side == 0 else j
                    to = y if side == 0 else RADIUS - 1 - y
                    moved = strip if at == to else pltpu.roll(strip, (to - at) % lz, 1)
                    total_y = total_y + jnp.where(lax.rem(lane, 4) == to, TAPS[RADIUS + far] * moved, 0.0)
            st_sum[side, quarter] = total_y

    def add_strips(k, _):
        for b in range(4):
            i = k * 4 + b
            at = i + n // 2 - 2
            quarter, q = at // (n // 2), lax.rem(at, n // 2)
            mine_y = slot == q
            low_y = pltpu.roll(jnp.where(mine_y, st_sum[0, quarter], 0.0), lz - 4 * q, 1)
            high_y = pltpu.roll(jnp.where(mine_y, st_sum[1, quarter], 0.0), lz + ly - RADIUS - 4 * q, 1)
            acc = yf[i] + low_y + high_y
            yf[i] = acc
            yr[i] = pltpu.roll(acc, ly, 1)
        return 0

    lax.fori_loop(0, (n + 4) // 4, add_strips, 0)
    first_half = lane < ly

    def along_x(k, _):
        for b in range(4):
            p = k * 4 + b
            i = p + 2
            near = yr[i] + jnp.where(first_half, yr[i - 1], yr[i + 1])
            far = jnp.where(first_half, yr[i - 2] + yr[i + 1], yr[i - 1] + yr[i + 2])
            acc = TAPS[RADIUS] * yf[i] + TAPS[RADIUS + 1] * near
            fc[p] = acc + TAPS[RADIUS + 2] * (yf[i - 1] + yf[i + 1]) + TAPS[RADIUS + 3] * far
        return 0

    lax.fori_loop(0, n // 4, along_x, 0)
    rows_per = lz // ly

    def finish(t, _):
        for b in range(BATCH):
            p = t * BATCH + b
            state = fc[p]
            hi = state.astype(BF16).astype(F32)
            stack = jnp.concatenate([hi, state - hi, hi, jnp.zeros((8, lz), F32)], axis=0)
            add = dot(jnp.transpose(stack).astype(BF16), vmap[...], 1, 0).reshape(rows_per, ly, lz)
            at = pl.ds(p * rows_per, rows_per)
            fm[at] = (fm[at] + add) * scale[at]
        return 0

    lax.fori_loop(0, n // BATCH, finish, 0)


def last(full, comp_in, out_hbm, comp_out, sem):
    step = full.shape[0] // PIECES

    def out_copy(k):
        rows = pl.ds(k * step, step)
        return pltpu.make_async_copy(full.at[rows], out_hbm.at[rows], sem.at[k])

    for k in range(PIECES):
        out_copy(k).start()
    for c in range(CASES):
        comp_out[c] = jnp.sum(comp_in[0:1, c : c + 1])
    for k in range(PIECES):
        out_copy(k).wait()


def local_step(sizes, density, design_mask, energy, decay, case_index, case_weight):
    n, ngx, ngy, lx, ly, lz, cells = sizes
    groups = lx // XG
    per = XG * ly
    others = ngx * ngy - 1
    dma = pltpu.SemaphoreType.DMA
    anywhere = pl.BlockSpec(memory_space=pltpu.HBM)
    smem = pl.BlockSpec(memory_space=pltpu.SMEM)
    vmem = pl.BlockSpec(memory_space=pltpu.VMEM)
    state = pltpu.VMEM((n, 8, lz), F32)
    sent = pltpu.VMEM((n, 8, lz), BF16)
    full, comp = pl.pallas_call(
        functools.partial(kernel, sizes),
        out_shape=(
            jax.ShapeDtypeStruct((lx, ly, lz), F32),
            jax.ShapeDtypeStruct((1, lz), F32),
        ),
        in_specs=[anywhere, anywhere, anywhere, vmem, smem, smem],
        out_specs=(vmem,) * 2,
        scratch_shapes=[
            pltpu.VMEM((lx, ly, lz), F32),
            pltpu.VMEM((lx, ly, lz), jnp.int32),
            pltpu.VMEM((CASES, lx, ly, lz), BF16),
            pltpu.VMEM((CASES, lz, lz), F32),
            pltpu.VMEM((groups, 2 * CASES, per, lz), BF16),
            pltpu.VMEM((2 * CASES * lz, 2 * lz), BF16),
            pltpu.VMEM((32, 2 * CASES * lz), BF16),
            pltpu.VMEM((lx + 2 * RADIUS, ly + 2 * YO, lz), F32),
            pltpu.VMEM((XG, ly + 2 * YO, lz), F32),
            pltpu.VMEM((lx, ly, lz), F32),
            state,
            pltpu.VMEM((32, lz), BF16),
            state,
            pltpu.VMEM((n + 4, 8, lz), F32),
            pltpu.VMEM((1, lz), F32),
            pltpu.VMEM((n, 1, lz), F32),
            state,
            state,
            sent,
            sent,
            state,
            sent,
            pltpu.VMEM((n + 4, 8, lz), BF16),
            pltpu.VMEM((n + 4, 8, lz), F32),
            pltpu.VMEM((n + 4, 8, lz), F32),
            pltpu.VMEM((1, lz), F32),
            pltpu.VMEM((others, 1, lz), F32),
            pltpu.VMEM((1, lz), F32),
            pltpu.VMEM((n, 1, lz), F32),
            pltpu.VMEM((RADIUS, ly, lz), BF16),
            pltpu.VMEM((RADIUS, ly, lz), BF16),
            pltpu.VMEM((2, RADIUS, lx, lz), BF16),
            pltpu.VMEM((2, RADIUS, lx, lz), BF16),
            pltpu.VMEM((2, RADIUS, RADIUS, lz), BF16),
            pltpu.VMEM((2, RADIUS, RADIUS, lz), BF16),
            pltpu.VMEM((2, 2, 8, lz), F32),
            pltpu.VMEM((2, 4, 8, lz), F32),
            pltpu.VMEM((2, 4, 8, lz), F32),
            dma((3, groups)),
            dma(()),
            dma(()),
            dma(()),
            dma(()),
            dma(()),
            dma(()),
            dma((others,)),
            dma((others,)),
            dma(()),
            dma(()),
            dma(()),
            dma(()),
            dma((2,)),
            dma((2,)),
            dma((2,)),
            dma((2,)),
            dma(()),
            dma(()),
            dma((2,)),
            dma((2,)),
            dma((2,)),
            dma((2,)),
        ],
        compiler_params=pltpu.CompilerParams(
            collective_id=0, has_side_effects=True, vmem_limit_bytes=40 * 1024 * 1024
        ),
        name="states",
    )(*(pltpu.with_memory_space_constraint(v, pltpu.HBM) for v in (density, design_mask, energy, decay, case_index, case_weight)))
    return pl.pallas_call(
        last,
        out_shape=(
            jax.ShapeDtypeStruct((lx, ly, lz), F32),
            jax.ShapeDtypeStruct((CASES,), F32),
        ),
        in_specs=[vmem] * 2,
        out_specs=(anywhere, smem),
        scratch_shapes=[dma((PIECES,))],
        compiler_params=pltpu.CompilerParams(vmem_limit_bytes=20 * 1024 * 1024),
        name="result",
    )(full, comp)


def solution(mesh):
    shape = mesh.shape
    n, ngx, ngy = shape["gz"], shape["gx"], shape["gy"]

    def whole(density, design_mask, energy, decay, case_index, case_weight):
        nx, ny, nz = density.shape
        sizes = (n, ngx, ngy, nx // ngx, ny // ngy, nz // n, nx * ny * nz)
        return jax.shard_map(
            functools.partial(local_step, sizes),
            mesh=mesh,
            in_specs=(
                P("gx", "gy", "gz"), P("gx", "gy", "gz"), P(None, "gx", "gy", "gz"), P(None, "gz"), P(), P(),
            ),
            out_specs=(P("gx", "gy", "gz"), P()),
            check_vma=False,
        )(density, design_mask, energy, decay, case_index, case_weight)

    return whole
```

```python
import functools
import math

import jax
import jax.numpy as jnp
from jax import lax
from jax.experimental import pallas as pl
from jax.experimental.pallas import tpu as pltpu
from jax.sharding import PartitionSpec as P

CASES = 4
RADIUS = 3
F32 = jnp.float32
BF16 = jnp.bfloat16
MESH = pl.DeviceIdType.MESH
HIGH = lax.Precision.HIGHEST
XG = 8
BATCH = 16
PIECES = 8
EARLY = 4
YO = 8

_raw = [math.exp(-2.0 * k * k / (RADIUS * RADIUS)) for k in range(-RADIUS, RADIUS + 1)]
TAPS = [t / sum(_raw) for t in _raw]


def dot(a, b, ca, cb, precision=None):
    return lax.dot_general(a, b, (((ca,), (cb,)), ((), ())), precision=precision, preferred_element_type=F32)


def split(value):
    hi = value.astype(BF16)
    return hi, (value - hi.astype(F32)).astype(BF16)


def taps(get):
    acc = TAPS[RADIUS] * get(RADIUS)
    for t in range(RADIUS):
        acc = acc + TAPS[t] * (get(t) + get(2 * RADIUS - t))
    return acc


def kernel(
    sizes, dens_hbm, mask_hbm, en_hbm, decay_ref, index_ref, weight_ref,
    fm, comp_out,
    dens, mask, en, fwd, lhs, maps, coef, ext, tmp, scale, fc, vmap, inv, cf,
    consts_out, consts_in, gain, mix, fh_out, fh_in, fin, carry_out, cx, yf, yr,
    cs_out, cs_in, ct_out, ct_in, xs_out, xs_in, ys_out, ys_in, ds_out, ds_in, st_out, st_in, st_sum,
    load_sem, cst_s, cst_r, ph1_s, ph1_r, ph2_s, ph2_r, cs_s, cs_r, ct_s, ct_r,
    xs_s, xs_r, ys_s, ys_r, ds_s, ds_r, cb_s, cb_r, st_s, st_r, dg_s, dg_r,
):
    n, ngx, ngy, lx, ly, lz, cells = sizes
    groups = lx // XG
    per = XG * ly
    blocks = per // lz
    gz, gx, gy = lax.axis_index("gz"), lax.axis_index("gx"), lax.axis_index("gy")
    others = ngx * ngy - 1
    mine = gz // blocks

    def peer(k):
        flat = lax.rem(gx * ngy + gy + 1 + k, ngx * ngy)
        return {"gz": gz, "gx": flat // ngy, "gy": lax.rem(flat, ngy)}

    def group_at(i):
        j = (i + 1) // 2
        off = jnp.where(lax.rem(i, 2) == 1, groups // 2 - j, groups // 2 + j)
        return lax.rem(mine + off, groups)

    def each_far(body):
        for k in sorted(range(1, n), key=lambda k: -min(k // blocks, (n - k) // blocks)):
            body(jnp.where(gz + k >= n, gz + k - n, gz + k))

    def end(ref, sem):
        pltpu.make_async_copy(ref, ref, sem).wait()

    for i in (0, 1, n + 2, n + 3):
        cx[i] = jnp.zeros((8, lz), BF16)
    st_in[...] = jnp.zeros_like(st_in)

    def loads(k):
        rows = pl.ds(k * XG, XG)
        return (
            pltpu.make_async_copy(dens_hbm.at[rows], dens.at[rows], load_sem.at[0, k]),
            pltpu.make_async_copy(mask_hbm.at[rows], mask.at[rows], load_sem.at[1, k]),
            pltpu.make_async_copy(en_hbm.at[:, rows], en.at[:, rows], load_sem.at[2, k]),
        )

    def start_loads(i, _):
        for copy in loads(group_at(i)):
            copy.start()
        return 0

    lax.fori_loop(0, 2, start_loads, 0)
    barrier = pltpu.get_barrier_semaphore()
    each_far(lambda p: pl.semaphore_signal(barrier, inc=1, device_id={"gz": p}, device_id_type=MESH))
    for k in range(others):
        pl.semaphore_signal(barrier, inc=1, device_id=peer(k), device_id_type=MESH)
    lax.fori_loop(2, groups, start_loads, 0)

    decay = jnp.concatenate([decay_ref[...], decay_ref[...]], axis=0)
    logs = jnp.log(decay)
    row = lax.broadcasted_iota(jnp.int32, (lz, lz), 0)
    col = lax.broadcasted_iota(jnp.int32, (lz, lz), 1)
    low, high = row <= col, row >= col
    up = dot(logs, low.astype(F32), 1, 0, HIGH)
    down = dot(logs, high.astype(F32), 1, 0, HIGH)
    keep = 1.0 - decay
    columns = jnp.transpose(jnp.concatenate([up, down, keep, keep], axis=0))
    total = up[:, lz - 1 : lz]
    fwd_last = jnp.exp(total - up) * keep
    first = jnp.exp(down[:, 0:1] - down) * keep
    lead = jnp.exp(up)
    trail = jnp.exp(down)
    rows8 = lax.broadcasted_iota(jnp.int32, (8, lz), 0)
    rows16 = lax.broadcasted_iota(jnp.int32, (16, lz), 0)
    lane = lax.broadcasted_iota(jnp.int32, (8, lz), 1)
    couple = jnp.sum(first * lead, axis=1, keepdims=True)
    across = jnp.where(rows8 == lane, jnp.exp(total), jnp.where(rows8 + 8 == lane, couple, 0.0))
    consts_out[...] = jnp.sum(across, axis=0, keepdims=True)
    consts_in[gz] = consts_out[...]

    for c in range(CASES):
        fwd_t = jnp.where(low, jnp.exp(jnp.where(low, up[c : c + 1] - columns[:, c : c + 1], 0.0)), 0.0)
        fwd_t = fwd_t * columns[:, 16 + c : 17 + c]
        fwd[c] = fwd_t
        hrow = dot(first, fwd_t, 1, 1, HIGH)
        cblock = jnp.where(rows8 == c, fwd_last, 0.0)
        cblock = jnp.where(rows8 == c + CASES, hrow, cblock)
        chi = cblock.astype(BF16).astype(F32)
        pair = jnp.concatenate([chi, cblock - chi], axis=0).astype(BF16)
        for half in range(2):
            at = (2 * c + half) * lz
            coef[0:16, at : at + lz] = pair
            coef[16:32, at : at + lz] = (rows16 == c).astype(F32).astype(BF16)

    spots = lane.astype(F32) * 0.6180339887 + rows8.astype(F32) * 0.3247179572

    def stretch(p):
        phase = spots + jnp.asarray(p, jnp.int32).astype(F32) * 0.7548776662
        return 1.0 + (phase - jnp.floor(phase))

    def operand(k):
        return jnp.concatenate([lhs[k, c] for c in range(2 * CASES)], axis=1)

    def local(at, sums):
        k = group_at(at)
        for copy in loads(k):
            copy.wait()
        for i in range(XG):
            x = k * XG + i
            d, m = dens[x], mask[x]
            dense = jnp.where(m == 1, 0.001, jnp.where(m == 2, 1.0, d))
            cube = dense * dense * dense
            for c in range(CASES):
                hi, lo = split(cube * en[c, x].astype(F32))
                lhs[k, 2 * c, i * ly : (i + 1) * ly] = hi
                lhs[k, 2 * c + 1, i * ly : (i + 1) * ly] = lo
        fh = dot(coef[...], operand(k), 1, 1)
        for b in range(blocks):
            piece = fh[:, b * lz : (b + 1) * lz]
            fh_out[k * blocks + b] = ((piece[0:8] + piece[8:16]) * stretch(k * blocks + b)).astype(BF16)
            sums = sums + piece[16:24]
        return sums

    def to_slab(src, dst, send, recv, k):
        return pltpu.make_async_remote_copy(
            src_ref=src, dst_ref=dst, send_sem=send, recv_sem=recv,
            device_id={"gz": k}, device_id_type=MESH,
        )

    def consts_copy(src, dst):
        return to_slab(consts_out, consts_in.at[src], cst_s, cst_r, dst)

    def ph1_copy(src, dst):
        return to_slab(fh_out.at[dst], fh_in.at[src], ph1_s, ph1_r, dst)

    def ph2_copy(src, dst):
        return to_slab(carry_out.at[dst], cx.at[2 + src], ph2_s, ph2_r, dst)

    def ct_copy(src, dst):
        return to_slab(ct_out, ct_in.at[src], ct_s, ct_r, dst)

    def send_group(at):
        for b in range(blocks):
            p = group_at(at) * blocks + b

            @pl.when(p != gz)
            def _():
                ph1_copy(gz, p).start()

    sums = lax.fori_loop(0, EARLY, local, jnp.zeros((8, lz), F32))
    pl.semaphore_wait(barrier, n - 1 + others)
    for at in range(EARLY):
        send_group(at)
    each_far(lambda p: consts_copy(gz, p).start())

    def local_send(at, sums):
        sums = local(at, sums)
        send_group(at)
        return sums

    sums = lax.fori_loop(EARLY, groups, local_send, sums)
    fh_in[gz] = fh_out[gz]

    sums = jnp.sum(sums, axis=1, keepdims=True)
    part = jnp.sum(jnp.where(rows8 == lane, sums, 0.0), axis=0, keepdims=True)
    cs_out[...] = part

    def cs_copy(k):
        return pltpu.make_async_remote_copy(
            src_ref=cs_out, dst_ref=cs_in.at[k], send_sem=cs_s.at[k], recv_sem=cs_r.at[k],
            device_id=peer(k), device_id_type=MESH,
        )

    for k in range(others):
        cs_copy(k).start()

    vals = jnp.zeros((8, lz), F32)
    for c in range(CASES):
        wc = weight_ref[index_ref[c]] * -3.0
        bwd_t = jnp.where(high, jnp.exp(jnp.where(high, down[c : c + 1] - columns[:, 8 + c : 9 + c], 0.0)), 0.0)
        bwd_t = bwd_t * columns[:, 16 + c : 17 + c]
        hi, lo = split(dot(fwd[c], bwd_t, 1, 0, HIGH) * wc)
        for half in range(2):
            at = (2 * c + half) * lz
            maps[at : at + lz, 0:lz] = hi
            maps[at : at + lz, lz : 2 * lz] = lo
        lead_map = dot(lead, bwd_t, 1, 0, HIGH)
        vals = jnp.where(rows8 == c, lead_map * wc, vals)
        vals = jnp.where(rows8 == c + CASES, trail * wc, vals)
    vhi = vals.astype(BF16).astype(F32)
    vmap[...] = jnp.concatenate([vhi, vhi, vals - vhi, jnp.zeros((8, lz), F32)], axis=0).astype(BF16)

    for j in range(RADIUS):
        ext[j] = jnp.zeros((ly + 2 * YO, lz), F32)
        ext[RADIUS + lx + j] = jnp.zeros((ly + 2 * YO, lz), F32)
    ext[:, 0:YO] = jnp.zeros((lx + 2 * RADIUS, YO, lz), F32)
    ext[:, YO + ly :] = jnp.zeros((lx + 2 * RADIUS, YO, lz), F32)

    def smoothed(k, _):
        full = dot(operand(k), maps[...], 1, 0)
        full = full[:, :lz] + full[:, lz:]
        ext[pl.ds(RADIUS + k * XG, XG), YO : YO + ly, :] = full.reshape(XG, ly, lz)
        for i in range(XG):
            x = k * XG + i
            scale[x] = jnp.where(mask[x] == 0, 1.0 / jnp.maximum(dens[x], 0.1), 0.0)
        return 0

    lax.fori_loop(0, groups, smoothed, 0)

    xs_at = jnp.where(gx == 0, lx - RADIUS, 0)
    for j in range(RADIUS):
        xs_out[j] = ext[RADIUS + xs_at + j, YO : YO + ly, :].astype(BF16)
    for side in range(2):
        for j in range(RADIUS):
            y = YO + (j if side == 0 else ly - RADIUS + j)
            ys_out[side, j] = ext[RADIUS : RADIUS + lx, y, :].astype(BF16)
            ds_out[side, j] = ext[pl.ds(RADIUS + xs_at, RADIUS), y, :].astype(BF16)

    def beside(src, dst, send, recv, where):
        return pltpu.make_async_remote_copy(
            src_ref=src, dst_ref=dst, send_sem=send, recv_sem=recv, device_id=where, device_id_type=MESH
        )

    def x_copy():
        return beside(xs_out, xs_in, xs_s, xs_r, {"gx": 1 - gx})

    def y_copy(side, to):
        return beside(ys_out.at[side], ys_in.at[1 - side], ys_s.at[side], ys_r.at[1 - side], {"gy": to})

    def d_copy(side, to):
        where = {"gx": 1 - gx, "gy": to}
        return beside(ds_out.at[side], ds_in.at[1 - side], ds_s.at[side], ds_r.at[1 - side], where)

    def blocks_copy():
        src = jnp.where(gx == 0, n, 2)
        dst = jnp.where(gx == 0, 0, n + 2)
        return beside(cx.at[pl.ds(src, 2)], cx.at[pl.ds(dst, 2)], cb_s, cb_r, {"gx": 1 - gx})

    def blocks_arrive():
        dst = jnp.where(gx == 0, n + 2, 0)
        return beside(cx.at[pl.ds(dst, 2)], cx.at[pl.ds(dst, 2)], cb_s, cb_r, {"gx": 1 - gx})

    def strip_copy(side, to):
        where = {"gy": to}
        return beside(st_out.at[side], st_in.at[1 - side, 1:3], st_s.at[side], st_r.at[1 - side], where)

    def corner_copy(side, to):
        where = {"gx": 1 - gx, "gy": to}
        dst = st_in.at[1 - side, jnp.where(gx == 0, 0, 3)]
        return beside(st_out.at[side, 1 - gx], dst, dg_s.at[side], dg_r.at[1 - side], where)

    def corner_arrive(side, to):
        where = {"gx": 1 - gx, "gy": to}
        dst = st_in.at[side, jnp.where(gx == 0, 3, 0)]
        return beside(st_out.at[side, 1 - gx], dst, dg_s.at[side], dg_r.at[side], where)

    def sides(body):
        @pl.when(gy > 0)
        def _():
            body(0, gy - 1)

        @pl.when(gy < ngy - 1)
        def _():
            body(1, gy + 1)

    x_copy().start()

    def send_halo(side, to):
        y_copy(side, to).start()
        d_copy(side, to).start()

    sides(send_halo)

    for p in range(n):
        inv[p] = 1.0 / stretch(p)
    end(ct_in.at[0 : n - 1], cst_r)
    spread = jnp.transpose(jnp.concatenate([consts_in[s] for s in range(n)], axis=0))
    for s in range(n):
        gain[s] = jnp.broadcast_to(spread[0:8, s : s + 1], (8, lz))
        mix[s] = jnp.broadcast_to(spread[8:16, s : s + 1], (8, lz))
    end(fh_in.at[0 : n - 1], ph1_r)
    shrink, widen = 1.0 / stretch(gz), stretch(gz)
    state = jnp.zeros((8, lz), F32)
    for s in range(n):
        fin[s] = state
        state = gain[s] * state + fh_in[s].astype(F32) * shrink
    state = jnp.zeros((8, lz), F32)
    for s in reversed(range(n)):
        entering = fin[s]
        carry_out[s] = (jnp.where(rows8 < CASES, entering, state) * widen).astype(BF16)
        state = gain[s] * state + (fh_in[s].astype(F32) * shrink + mix[s] * pltpu.roll(entering, CASES, 0))
    each_far(lambda p: ph2_copy(gz, p).start())
    cx[2 + gz] = carry_out[gz]
    for k in range(others):
        cs_copy(k).wait_recv()
        part = part + cs_in[k]
    ct_out[...] = part
    ct_in[gz] = part
    each_far(lambda p: ct_copy(gz, p).start())


    halo_x = jnp.where(gx == 0, RADIUS + lx, 0)
    x_copy().wait()
    ext[pl.ds(halo_x, RADIUS), YO : YO + ly, :] = xs_in[...].astype(F32)

    def take(side, to):
        for copy in (y_copy, d_copy):
            copy(side, to).wait_send()
            copy(1 - side, to).wait_recv()
        for j in range(RADIUS):
            y = YO + (j - RADIUS if side == 0 else ly + j)
            ext[RADIUS : RADIUS + lx, y, :] = ys_in[side, j].astype(F32)
            ext[pl.ds(halo_x, RADIUS), y, :] = ds_in[side, j].astype(F32)

    sides(take)

    def filtered(k, _):
        for i in range(XG):
            x = k * XG + i
            tmp[i] = taps(lambda t: ext[x + t])
            fm[x] = taps(lambda t: tmp[i, YO - RADIUS + t : YO - RADIUS + t + ly, :])
        return 0

    lax.fori_loop(0, groups, filtered, 0)

    end(fh_in.at[0 : n - 1], ph2_r)
    blocks_copy().start()
    for p in range(n):
        cf[2 + p] = cx[2 + p].astype(F32) * inv[p]
    half_y = lax.rem(lane, ly)
    slot = half_y // 4
    for side in range(2):
        y0 = 0 if side == 0 else ly - RADIUS
        for half in range(2):
            packed = jnp.zeros((8, lz), F32)
            for q in range(n // 2):
                moved = pltpu.roll(cf[2 + half * (n // 2) + q], (4 * q - y0) % lz, 1)
                packed = jnp.where(slot == q, moved, packed)
            st_out[side, half] = packed

    def send_strip(side, to):
        strip_copy(side, to).start()
        corner_copy(side, to).start()

    sides(send_strip)
    def add_ct(s, state):
        return state + ct_in[s]

    end(ct_in.at[0 : n - 1], ct_r)
    comp_out[...] = lax.fori_loop(0, n, add_ct, jnp.zeros((1, lz), F32)) * (1.0 / cells)

    for sem in (ph1_s, ph2_s):
        end(fh_in.at[0 : n - 1], sem)
    for sem in (cst_s, ct_s):
        end(ct_in.at[0 : n - 1], sem)
    for k in range(others):
        cs_copy(k).wait_send()

    def along_y(k, _):
        for b in range(4):
            i = k * 4 + b
            state = cf[2 + i]
            acc = TAPS[RADIUS] * state
            for t in range(1, RADIUS + 1):
                down_y = jnp.where(half_y >= t, pltpu.roll(state, t, 1), 0.0)
                up_y = jnp.where(half_y < ly - t, pltpu.roll(state, lz - t, 1), 0.0)
                acc = acc + TAPS[RADIUS + t] * (down_y + up_y)
            yf[2 + i] = acc
        return 0

    lax.fori_loop(0, n // 4, along_y, 0)

    blocks_copy().wait_send()
    blocks_arrive().wait_recv()
    for i in (0, 1, n + 2, n + 3):
        state = cx[i].astype(F32) * inv[(i - 2) % n]
        acc = TAPS[RADIUS] * state
        for t in range(1, RADIUS + 1):
            down_y = jnp.where(half_y >= t, pltpu.roll(state, t, 1), 0.0)
            up_y = jnp.where(half_y < ly - t, pltpu.roll(state, lz - t, 1), 0.0)
            acc = acc + TAPS[RADIUS + t] * (down_y + up_y)
        yf[i] = acc

    def take_strip(side, to):
        strip_copy(side, to).wait_send()
        corner_copy(side, to).wait_send()
        strip_copy(1 - side, to).wait_recv()
        corner_arrive(side, to).wait_recv()

    sides(take_strip)

    for side in range(2):
        for quarter in range(4):
            strip = st_in[side, quarter]
            total_y = jnp.zeros((8, lz), F32)
            for y in range(RADIUS):
                for j in range(RADIUS):
                    far = y + j + 1
                    if far > RADIUS:
                        continue
                    at = RADIUS - 1 - j if side == 0 else j
                    to = y if side == 0 else RADIUS - 1 - y
                    moved = strip if at == to else pltpu.roll(strip, (to - at) % lz, 1)
                    total_y = total_y + jnp.where(lax.rem(lane, 4) == to, TAPS[RADIUS + far] * moved, 0.0)
            st_sum[side, quarter] = total_y

    for i in range(n + 4):
        at = i + n // 2 - 2
        quarter, q = at // (n // 2), at % (n // 2)
        mine_y = slot == q
        low_y = pltpu.roll(jnp.where(mine_y, st_sum[0, quarter], 0.0), (-4 * q) % lz, 1)
        high_y = pltpu.roll(jnp.where(mine_y, st_sum[1, quarter], 0.0), (ly - RADIUS - 4 * q) % lz, 1)
        acc = yf[i] + low_y + high_y
        yf[i] = acc
        yr[i] = pltpu.roll(acc, ly, 1)
    first_half = lane < ly
    for p in range(n):
        i = p + 2
        near = yr[i] + jnp.where(first_half, yr[i - 1], yr[i + 1])
        far = jnp.where(first_half, yr[i - 2] + yr[i + 1], yr[i - 1] + yr[i + 2])
        acc = TAPS[RADIUS] * yf[i] + TAPS[RADIUS + 1] * near
        fc[p] = acc + TAPS[RADIUS + 2] * (yf[i - 1] + yf[i + 1]) + TAPS[RADIUS + 3] * far
    rows_per = lz // ly

    def finish(t, _):
        for b in range(BATCH):
            p = t * BATCH + b
            state = fc[p]
            hi = state.astype(BF16).astype(F32)
            stack = jnp.concatenate([hi, state - hi, hi, jnp.zeros((8, lz), F32)], axis=0)
            add = dot(jnp.transpose(stack).astype(BF16), vmap[...], 1, 0).reshape(rows_per, ly, lz)
            at = pl.ds(p * rows_per, rows_per)
            fm[at] = (fm[at] + add) * scale[at]
        return 0

    lax.fori_loop(0, n // BATCH, finish, 0)


def last(full, comp_in, out_hbm, comp_out, sem):
    step = full.shape[0] // PIECES

    def out_copy(k):
        rows = pl.ds(k * step, step)
        return pltpu.make_async_copy(full.at[rows], out_hbm.at[rows], sem.at[k])

    for k in range(PIECES):
        out_copy(k).start()
    for c in range(CASES):
        comp_out[c] = jnp.sum(comp_in[0:1, c : c + 1])
    for k in range(PIECES):
        out_copy(k).wait()


def local_step(sizes, density, design_mask, energy, decay, case_index, case_weight):
    n, ngx, ngy, lx, ly, lz, cells = sizes
    groups = lx // XG
    per = XG * ly
    others = ngx * ngy - 1
    dma = pltpu.SemaphoreType.DMA
    anywhere = pl.BlockSpec(memory_space=pltpu.HBM)
    smem = pl.BlockSpec(memory_space=pltpu.SMEM)
    vmem = pl.BlockSpec(memory_space=pltpu.VMEM)
    state = pltpu.VMEM((n, 8, lz), F32)
    sent = pltpu.VMEM((n, 8, lz), BF16)
    full, comp = pl.pallas_call(
        functools.partial(kernel, sizes),
        out_shape=(
            jax.ShapeDtypeStruct((lx, ly, lz), F32),
            jax.ShapeDtypeStruct((1, lz), F32),
        ),
        in_specs=[anywhere, anywhere, anywhere, vmem, smem, smem],
        out_specs=(vmem,) * 2,
        scratch_shapes=[
            pltpu.VMEM((lx, ly, lz), F32),
            pltpu.VMEM((lx, ly, lz), jnp.int32),
            pltpu.VMEM((CASES, lx, ly, lz), BF16),
            pltpu.VMEM((CASES, lz, lz), F32),
            pltpu.VMEM((groups, 2 * CASES, per, lz), BF16),
            pltpu.VMEM((2 * CASES * lz, 2 * lz), BF16),
            pltpu.VMEM((32, 2 * CASES * lz), BF16),
            pltpu.VMEM((lx + 2 * RADIUS, ly + 2 * YO, lz), F32),
            pltpu.VMEM((XG, ly + 2 * YO, lz), F32),
            pltpu.VMEM((lx, ly, lz), F32),
            state,
            pltpu.VMEM((32, lz), BF16),
            state,
            pltpu.VMEM((n + 4, 8, lz), F32),
            pltpu.VMEM((1, lz), F32),
            pltpu.VMEM((n, 1, lz), F32),
            state,
            state,
            sent,
            sent,
            state,
            sent,
            pltpu.VMEM((n + 4, 8, lz), BF16),
            pltpu.VMEM((n + 4, 8, lz), F32),
            pltpu.VMEM((n + 4, 8, lz), F32),
            pltpu.VMEM((1, lz), F32),
            pltpu.VMEM((others, 1, lz), F32),
            pltpu.VMEM((1, lz), F32),
            pltpu.VMEM((n, 1, lz), F32),
            pltpu.VMEM((RADIUS, ly, lz), BF16),
            pltpu.VMEM((RADIUS, ly, lz), BF16),
            pltpu.VMEM((2, RADIUS, lx, lz), BF16),
            pltpu.VMEM((2, RADIUS, lx, lz), BF16),
            pltpu.VMEM((2, RADIUS, RADIUS, lz), BF16),
            pltpu.VMEM((2, RADIUS, RADIUS, lz), BF16),
            pltpu.VMEM((2, 2, 8, lz), F32),
            pltpu.VMEM((2, 4, 8, lz), F32),
            pltpu.VMEM((2, 4, 8, lz), F32),
            dma((3, groups)),
            dma(()),
            dma(()),
            dma(()),
            dma(()),
            dma(()),
            dma(()),
            dma((others,)),
            dma((others,)),
            dma(()),
            dma(()),
            dma(()),
            dma(()),
            dma((2,)),
            dma((2,)),
            dma((2,)),
            dma((2,)),
            dma(()),
            dma(()),
            dma((2,)),
            dma((2,)),
            dma((2,)),
            dma((2,)),
        ],
        compiler_params=pltpu.CompilerParams(
            collective_id=0, has_side_effects=True, vmem_limit_bytes=40 * 1024 * 1024
        ),
        name="states",
    )(*(pltpu.with_memory_space_constraint(v, pltpu.HBM) for v in (density, design_mask, energy, decay, case_index, case_weight)))
    return pl.pallas_call(
        last,
        out_shape=(
            jax.ShapeDtypeStruct((lx, ly, lz), F32),
            jax.ShapeDtypeStruct((CASES,), F32),
        ),
        in_specs=[vmem] * 2,
        out_specs=(anywhere, smem),
        scratch_shapes=[dma((PIECES,))],
        compiler_params=pltpu.CompilerParams(vmem_limit_bytes=20 * 1024 * 1024),
        name="result",
    )(full, comp)


def solution(mesh):
    shape = mesh.shape
    n, ngx, ngy = shape["gz"], shape["gx"], shape["gy"]

    def whole(density, design_mask, energy, decay, case_index, case_weight):
        nx, ny, nz = density.shape
        sizes = (n, ngx, ngy, nx // ngx, ny // ngy, nz // n, nx * ny * nz)
        return jax.shard_map(
            functools.partial(local_step, sizes),
            mesh=mesh,
            in_specs=(
                P("gx", "gy", "gz"), P("gx", "gy", "gz"), P(None, "gx", "gy", "gz"), P(None, "gz"), P(), P(),
            ),
            out_specs=(P("gx", "gy", "gz"), P()),
            check_vma=False,
        )(density, design_mask, energy, decay, case_index, case_weight)

    return whole
```

```python
import functools
import math

import jax
import jax.numpy as jnp
from jax import lax
from jax.experimental import pallas as pl
from jax.experimental.pallas import tpu as pltpu
from jax.sharding import PartitionSpec as P

CASES = 4
RADIUS = 3
F32 = jnp.float32
BF16 = jnp.bfloat16
MESH = pl.DeviceIdType.MESH
HIGH = lax.Precision.HIGHEST
XG = 8
BATCH = 32
PIECES = 8
EARLY = 4
YO = 8

_raw = [math.exp(-2.0 * k * k / (RADIUS * RADIUS)) for k in range(-RADIUS, RADIUS + 1)]
TAPS = [t / sum(_raw) for t in _raw]


def dot(a, b, ca, cb, precision=None):
    return lax.dot_general(a, b, (((ca,), (cb,)), ((), ())), precision=precision, preferred_element_type=F32)


def split(value):
    hi = value.astype(BF16)
    return hi, (value - hi.astype(F32)).astype(BF16)


def taps(get):
    acc = TAPS[RADIUS] * get(RADIUS)
    for t in range(RADIUS):
        acc = acc + TAPS[t] * (get(t) + get(2 * RADIUS - t))
    return acc


def kernel(
    sizes, dens_hbm, mask_hbm, en_hbm, decay_ref, index_ref, weight_ref,
    fm, comp_out,
    dens, mask, en, fwd, lhs, maps, coef, ext, tmp, scale, fc, vmap, inv, cf,
    consts_out, consts_in, gain, mix, fh_out, fh_in, fin, carry_out, cx, yf, yr,
    cs_out, cs_in, ct_out, ct_in, xs_out, xs_in, ys_out, ys_in, ds_out, ds_in, st_out, st_in, st_sum,
    load_sem, cst_s, cst_r, ph1_s, ph1_r, ph2_s, ph2_r, cs_s, cs_r, ct_s, ct_r,
    xs_s, xs_r, ys_s, ys_r, ds_s, ds_r, cb_s, cb_r, st_s, st_r, dg_s, dg_r,
):
    n, ngx, ngy, lx, ly, lz, cells = sizes
    groups = lx // XG
    per = XG * ly
    blocks = per // lz
    gz, gx, gy = lax.axis_index("gz"), lax.axis_index("gx"), lax.axis_index("gy")
    others = ngx * ngy - 1
    mine = gz // blocks

    def peer(k):
        flat = lax.rem(gx * ngy + gy + 1 + k, ngx * ngy)
        return {"gz": gz, "gx": flat // ngy, "gy": lax.rem(flat, ngy)}

    def group_at(i):
        j = (i + 1) // 2
        off = jnp.where(lax.rem(i, 2) == 1, groups // 2 - j, groups // 2 + j)
        return lax.rem(mine + off, groups)

    def each_far(body):
        for k in sorted(range(1, n), key=lambda k: -min(k // blocks, (n - k) // blocks)):
            body(jnp.where(gz + k >= n, gz + k - n, gz + k))

    def end(ref, sem):
        pltpu.make_async_copy(ref, ref, sem).wait()

    for i in (0, 1, n + 2, n + 3):
        cx[i] = jnp.zeros((8, lz), BF16)
    st_in[...] = jnp.zeros_like(st_in)

    def loads(k):
        rows = pl.ds(k * XG, XG)
        return (
            pltpu.make_async_copy(dens_hbm.at[rows], dens.at[rows], load_sem.at[0, k]),
            pltpu.make_async_copy(mask_hbm.at[rows], mask.at[rows], load_sem.at[1, k]),
            pltpu.make_async_copy(en_hbm.at[:, rows], en.at[:, rows], load_sem.at[2, k]),
        )

    def start_loads(i, _):
        for copy in loads(group_at(i)):
            copy.start()
        return 0

    lax.fori_loop(0, 2, start_loads, 0)
    barrier = pltpu.get_barrier_semaphore()
    each_far(lambda p: pl.semaphore_signal(barrier, inc=1, device_id={"gz": p}, device_id_type=MESH))
    for k in range(others):
        pl.semaphore_signal(barrier, inc=1, device_id=peer(k), device_id_type=MESH)
    lax.fori_loop(2, groups, start_loads, 0)

    decay = jnp.concatenate([decay_ref[...], decay_ref[...]], axis=0)
    logs = jnp.log(decay)
    row = lax.broadcasted_iota(jnp.int32, (lz, lz), 0)
    col = lax.broadcasted_iota(jnp.int32, (lz, lz), 1)
    low, high = row <= col, row >= col
    up = dot(logs, low.astype(F32), 1, 0, HIGH)
    down = dot(logs, high.astype(F32), 1, 0, HIGH)
    keep = 1.0 - decay
    columns = jnp.transpose(jnp.concatenate([up, down, keep, keep], axis=0))
    total = up[:, lz - 1 : lz]
    fwd_last = jnp.exp(total - up) * keep
    first = jnp.exp(down[:, 0:1] - down) * keep
    lead = jnp.exp(up)
    trail = jnp.exp(down)
    rows8 = lax.broadcasted_iota(jnp.int32, (8, lz), 0)
    rows16 = lax.broadcasted_iota(jnp.int32, (16, lz), 0)
    lane = lax.broadcasted_iota(jnp.int32, (8, lz), 1)
    couple = jnp.sum(first * lead, axis=1, keepdims=True)
    across = jnp.where(rows8 == lane, jnp.exp(total), jnp.where(rows8 + 8 == lane, couple, 0.0))
    consts_out[...] = jnp.sum(across, axis=0, keepdims=True)
    consts_in[gz] = consts_out[...]

    for c in range(CASES):
        fwd_t = jnp.where(low, jnp.exp(jnp.where(low, up[c : c + 1] - columns[:, c : c + 1], 0.0)), 0.0)
        fwd_t = fwd_t * columns[:, 16 + c : 17 + c]
        fwd[c] = fwd_t
        hrow = dot(first, fwd_t, 1, 1, HIGH)
        cblock = jnp.where(rows8 == c, fwd_last, 0.0)
        cblock = jnp.where(rows8 == c + CASES, hrow, cblock)
        chi = cblock.astype(BF16).astype(F32)
        pair = jnp.concatenate([chi, cblock - chi], axis=0).astype(BF16)
        for half in range(2):
            at = (2 * c + half) * lz
            coef[0:16, at : at + lz] = pair
            coef[16:32, at : at + lz] = (rows16 == c).astype(F32).astype(BF16)

    spots = lane.astype(F32) * 0.6180339887 + rows8.astype(F32) * 0.3247179572

    def stretch(p):
        phase = spots + jnp.asarray(p, jnp.int32).astype(F32) * 0.7548776662
        return 1.0 + (phase - jnp.floor(phase))

    def operand(k):
        return jnp.concatenate([lhs[k, c] for c in range(2 * CASES)], axis=1)

    def local(at, sums):
        k = group_at(at)
        for copy in loads(k):
            copy.wait()
        for i in range(XG):
            x = k * XG + i
            d, m = dens[x], mask[x]
            dense = jnp.where(m == 1, 0.001, jnp.where(m == 2, 1.0, d))
            cube = dense * dense * dense
            for c in range(CASES):
                hi, lo = split(cube * en[c, x].astype(F32))
                lhs[k, 2 * c, i * ly : (i + 1) * ly] = hi
                lhs[k, 2 * c + 1, i * ly : (i + 1) * ly] = lo
        fh = dot(coef[...], operand(k), 1, 1)
        for b in range(blocks):
            piece = fh[:, b * lz : (b + 1) * lz]
            fh_out[k * blocks + b] = ((piece[0:8] + piece[8:16]) * stretch(k * blocks + b)).astype(BF16)
            sums = sums + piece[16:24]
        return sums

    def to_slab(src, dst, send, recv, k):
        return pltpu.make_async_remote_copy(
            src_ref=src, dst_ref=dst, send_sem=send, recv_sem=recv,
            device_id={"gz": k}, device_id_type=MESH,
        )

    def consts_copy(src, dst):
        return to_slab(consts_out, consts_in.at[src], cst_s, cst_r, dst)

    def ph1_copy(src, dst):
        return to_slab(fh_out.at[dst], fh_in.at[src], ph1_s, ph1_r, dst)

    def ph2_copy(src, dst):
        return to_slab(carry_out.at[dst], cx.at[2 + src], ph2_s, ph2_r, dst)

    def ct_copy(src, dst):
        return to_slab(ct_out, ct_in.at[src], ct_s, ct_r, dst)

    def send_group(at):
        for b in range(blocks):
            p = group_at(at) * blocks + b

            @pl.when(p != gz)
            def _():
                ph1_copy(gz, p).start()

    sums = lax.fori_loop(0, EARLY, local, jnp.zeros((8, lz), F32))
    pl.semaphore_wait(barrier, n - 1 + others)
    for at in range(EARLY):
        send_group(at)
    each_far(lambda p: consts_copy(gz, p).start())

    def local_send(at, sums):
        sums = local(at, sums)
        send_group(at)
        return sums

    sums = lax.fori_loop(EARLY, groups, local_send, sums)
    fh_in[gz] = fh_out[gz]

    sums = jnp.sum(sums, axis=1, keepdims=True)
    part = jnp.sum(jnp.where(rows8 == lane, sums, 0.0), axis=0, keepdims=True)
    cs_out[...] = part

    def cs_copy(k):
        return pltpu.make_async_remote_copy(
            src_ref=cs_out, dst_ref=cs_in.at[k], send_sem=cs_s.at[k], recv_sem=cs_r.at[k],
            device_id=peer(k), device_id_type=MESH,
        )

    for k in range(others):
        cs_copy(k).start()

    vals = jnp.zeros((8, lz), F32)
    for c in range(CASES):
        wc = weight_ref[index_ref[c]] * -3.0
        bwd_t = jnp.where(high, jnp.exp(jnp.where(high, down[c : c + 1] - columns[:, 8 + c : 9 + c], 0.0)), 0.0)
        bwd_t = bwd_t * columns[:, 16 + c : 17 + c]
        hi, lo = split(dot(fwd[c], bwd_t, 1, 0, HIGH) * wc)
        for half in range(2):
            at = (2 * c + half) * lz
            maps[at : at + lz, 0:lz] = hi
            maps[at : at + lz, lz : 2 * lz] = lo
        lead_map = dot(lead, bwd_t, 1, 0, HIGH)
        vals = jnp.where(rows8 == c, lead_map * wc, vals)
        vals = jnp.where(rows8 == c + CASES, trail * wc, vals)
    vhi = vals.astype(BF16).astype(F32)
    vmap[...] = jnp.concatenate([vhi, vhi, vals - vhi, jnp.zeros((8, lz), F32)], axis=0).astype(BF16)

    for j in range(RADIUS):
        ext[j] = jnp.zeros((ly + 2 * YO, lz), F32)
        ext[RADIUS + lx + j] = jnp.zeros((ly + 2 * YO, lz), F32)
    ext[:, 0:YO] = jnp.zeros((lx + 2 * RADIUS, YO, lz), F32)
    ext[:, YO + ly :] = jnp.zeros((lx + 2 * RADIUS, YO, lz), F32)

    def smoothed(k, _):
        full = dot(operand(k), maps[...], 1, 0)
        full = full[:, :lz] + full[:, lz:]
        ext[pl.ds(RADIUS + k * XG, XG), YO : YO + ly, :] = full.reshape(XG, ly, lz)
        for i in range(XG):
            x = k * XG + i
            scale[x] = jnp.where(mask[x] == 0, 1.0 / jnp.maximum(dens[x], 0.1), 0.0)
        return 0

    lax.fori_loop(0, groups, smoothed, 0)

    xs_at = jnp.where(gx == 0, lx - RADIUS, 0)
    for j in range(RADIUS):
        xs_out[j] = ext[RADIUS + xs_at + j, YO : YO + ly, :].astype(BF16)
    for side in range(2):
        for j in range(RADIUS):
            y = YO + (j if side == 0 else ly - RADIUS + j)
            ys_out[side, j] = ext[RADIUS : RADIUS + lx, y, :].astype(BF16)
            ds_out[side, j] = ext[pl.ds(RADIUS + xs_at, RADIUS), y, :].astype(BF16)

    def beside(src, dst, send, recv, where):
        return pltpu.make_async_remote_copy(
            src_ref=src, dst_ref=dst, send_sem=send, recv_sem=recv, device_id=where, device_id_type=MESH
        )

    def x_copy():
        return beside(xs_out, xs_in, xs_s, xs_r, {"gx": 1 - gx})

    def y_copy(side, to):
        return beside(ys_out.at[side], ys_in.at[1 - side], ys_s.at[side], ys_r.at[1 - side], {"gy": to})

    def d_copy(side, to):
        where = {"gx": 1 - gx, "gy": to}
        return beside(ds_out.at[side], ds_in.at[1 - side], ds_s.at[side], ds_r.at[1 - side], where)

    def blocks_copy():
        src = jnp.where(gx == 0, n, 2)
        dst = jnp.where(gx == 0, 0, n + 2)
        return beside(cx.at[pl.ds(src, 2)], cx.at[pl.ds(dst, 2)], cb_s, cb_r, {"gx": 1 - gx})

    def blocks_arrive():
        dst = jnp.where(gx == 0, n + 2, 0)
        return beside(cx.at[pl.ds(dst, 2)], cx.at[pl.ds(dst, 2)], cb_s, cb_r, {"gx": 1 - gx})

    def strip_copy(side, to):
        where = {"gy": to}
        return beside(st_out.at[side], st_in.at[1 - side, 1:3], st_s.at[side], st_r.at[1 - side], where)

    def corner_copy(side, to):
        where = {"gx": 1 - gx, "gy": to}
        dst = st_in.at[1 - side, jnp.where(gx == 0, 0, 3)]
        return beside(st_out.at[side, 1 - gx], dst, dg_s.at[side], dg_r.at[1 - side], where)

    def corner_arrive(side, to):
        where = {"gx": 1 - gx, "gy": to}
        dst = st_in.at[side, jnp.where(gx == 0, 3, 0)]
        return beside(st_out.at[side, 1 - gx], dst, dg_s.at[side], dg_r.at[side], where)

    def sides(body):
        @pl.when(gy > 0)
        def _():
            body(0, gy - 1)

        @pl.when(gy < ngy - 1)
        def _():
            body(1, gy + 1)

    x_copy().start()

    def send_halo(side, to):
        y_copy(side, to).start()
        d_copy(side, to).start()

    sides(send_halo)

    for p in range(n):
        inv[p] = 1.0 / stretch(p)
    end(ct_in.at[0 : n - 1], cst_r)
    spread = jnp.transpose(jnp.concatenate([consts_in[s] for s in range(n)], axis=0))
    for s in range(n):
        gain[s] = jnp.broadcast_to(spread[0:8, s : s + 1], (8, lz))
        mix[s] = jnp.broadcast_to(spread[8:16, s : s + 1], (8, lz))
    end(fh_in.at[0 : n - 1], ph1_r)
    shrink, widen = 1.0 / stretch(gz), stretch(gz)
    state = jnp.zeros((8, lz), F32)
    for s in range(n):
        fin[s] = state
        state = gain[s] * state + fh_in[s].astype(F32) * shrink
    state = jnp.zeros((8, lz), F32)
    for s in reversed(range(n)):
        entering = fin[s]
        carry_out[s] = (jnp.where(rows8 < CASES, entering, state) * widen).astype(BF16)
        state = gain[s] * state + (fh_in[s].astype(F32) * shrink + mix[s] * pltpu.roll(entering, CASES, 0))
    each_far(lambda p: ph2_copy(gz, p).start())
    cx[2 + gz] = carry_out[gz]
    for k in range(others):
        cs_copy(k).wait_recv()
        part = part + cs_in[k]
    ct_out[...] = part
    ct_in[gz] = part
    each_far(lambda p: ct_copy(gz, p).start())


    halo_x = jnp.where(gx == 0, RADIUS + lx, 0)
    x_copy().wait()
    ext[pl.ds(halo_x, RADIUS), YO : YO + ly, :] = xs_in[...].astype(F32)

    def take(side, to):
        for copy in (y_copy, d_copy):
            copy(side, to).wait_send()
            copy(1 - side, to).wait_recv()
        for j in range(RADIUS):
            y = YO + (j - RADIUS if side == 0 else ly + j)
            ext[RADIUS : RADIUS + lx, y, :] = ys_in[side, j].astype(F32)
            ext[pl.ds(halo_x, RADIUS), y, :] = ds_in[side, j].astype(F32)

    sides(take)

    def filtered(k, _):
        for i in range(XG):
            x = k * XG + i
            tmp[i] = taps(lambda t: ext[x + t])
            fm[x] = taps(lambda t: tmp[i, YO - RADIUS + t : YO - RADIUS + t + ly, :])
        return 0

    lax.fori_loop(0, groups, filtered, 0)

    end(fh_in.at[0 : n - 1], ph2_r)
    blocks_copy().start()
    for p in range(n):
        cf[2 + p] = cx[2 + p].astype(F32) * inv[p]
    half_y = lax.rem(lane, ly)
    slot = half_y // 4
    for side in range(2):
        y0 = 0 if side == 0 else ly - RADIUS
        for half in range(2):
            packed = jnp.zeros((8, lz), F32)
            for q in range(n // 2):
                moved = pltpu.roll(cf[2 + half * (n // 2) + q], (4 * q - y0) % lz, 1)
                packed = jnp.where(slot == q, moved, packed)
            st_out[side, half] = packed

    def send_strip(side, to):
        strip_copy(side, to).start()
        corner_copy(side, to).start()

    sides(send_strip)
    def add_ct(s, state):
        return state + ct_in[s]

    end(ct_in.at[0 : n - 1], ct_r)
    comp_out[...] = lax.fori_loop(0, n, add_ct, jnp.zeros((1, lz), F32)) * (1.0 / cells)

    for sem in (ph1_s, ph2_s):
        end(fh_in.at[0 : n - 1], sem)
    for sem in (cst_s, ct_s):
        end(ct_in.at[0 : n - 1], sem)
    for k in range(others):
        cs_copy(k).wait_send()

    def along_y(k, _):
        for b in range(4):
            i = k * 4 + b
            state = cf[2 + i]
            acc = TAPS[RADIUS] * state
            for t in range(1, RADIUS + 1):
                down_y = jnp.where(half_y >= t, pltpu.roll(state, t, 1), 0.0)
                up_y = jnp.where(half_y < ly - t, pltpu.roll(state, lz - t, 1), 0.0)
                acc = acc + TAPS[RADIUS + t] * (down_y + up_y)
            yf[2 + i] = acc
        return 0

    lax.fori_loop(0, n // 4, along_y, 0)

    blocks_copy().wait_send()
    blocks_arrive().wait_recv()
    for i in (0, 1, n + 2, n + 3):
        state = cx[i].astype(F32) * inv[(i - 2) % n]
        acc = TAPS[RADIUS] * state
        for t in range(1, RADIUS + 1):
            down_y = jnp.where(half_y >= t, pltpu.roll(state, t, 1), 0.0)
            up_y = jnp.where(half_y < ly - t, pltpu.roll(state, lz - t, 1), 0.0)
            acc = acc + TAPS[RADIUS + t] * (down_y + up_y)
        yf[i] = acc

    def take_strip(side, to):
        strip_copy(side, to).wait_send()
        corner_copy(side, to).wait_send()
        strip_copy(1 - side, to).wait_recv()
        corner_arrive(side, to).wait_recv()

    sides(take_strip)

    for side in range(2):
        for quarter in range(4):
            strip = st_in[side, quarter]
            total_y = jnp.zeros((8, lz), F32)
            for y in range(RADIUS):
                for j in range(RADIUS):
                    far = y + j + 1
                    if far > RADIUS:
                        continue
                    at = RADIUS - 1 - j if side == 0 else j
                    to = y if side == 0 else RADIUS - 1 - y
                    moved = strip if at == to else pltpu.roll(strip, (to - at) % lz, 1)
                    total_y = total_y + jnp.where(lax.rem(lane, 4) == to, TAPS[RADIUS + far] * moved, 0.0)
            st_sum[side, quarter] = total_y

    for i in range(n + 4):
        at = i + n // 2 - 2
        quarter, q = at // (n // 2), at % (n // 2)
        mine_y = slot == q
        low_y = pltpu.roll(jnp.where(mine_y, st_sum[0, quarter], 0.0), (-4 * q) % lz, 1)
        high_y = pltpu.roll(jnp.where(mine_y, st_sum[1, quarter], 0.0), (ly - RADIUS - 4 * q) % lz, 1)
        acc = yf[i] + low_y + high_y
        yf[i] = acc
        yr[i] = pltpu.roll(acc, ly, 1)
    first_half = lane < ly
    for p in range(n):
        i = p + 2
        near = yr[i] + jnp.where(first_half, yr[i - 1], yr[i + 1])
        far = jnp.where(first_half, yr[i - 2] + yr[i + 1], yr[i - 1] + yr[i + 2])
        acc = TAPS[RADIUS] * yf[i] + TAPS[RADIUS + 1] * near
        fc[p] = acc + TAPS[RADIUS + 2] * (yf[i - 1] + yf[i + 1]) + TAPS[RADIUS + 3] * far
    rows_per = lz // ly

    def finish(t, _):
        for b in range(BATCH):
            p = t * BATCH + b
            state = fc[p]
            hi = state.astype(BF16).astype(F32)
            stack = jnp.concatenate([hi, state - hi, hi, jnp.zeros((8, lz), F32)], axis=0)
            add = dot(jnp.transpose(stack).astype(BF16), vmap[...], 1, 0).reshape(rows_per, ly, lz)
            at = pl.ds(p * rows_per, rows_per)
            fm[at] = (fm[at] + add) * scale[at]
        return 0

    lax.fori_loop(0, n // BATCH, finish, 0)


def last(full, comp_in, out_hbm, comp_out, sem):
    step = full.shape[0] // PIECES

    def out_copy(k):
        rows = pl.ds(k * step, step)
        return pltpu.make_async_copy(full.at[rows], out_hbm.at[rows], sem.at[k])

    for k in range(PIECES):
        out_copy(k).start()
    for c in range(CASES):
        comp_out[c] = jnp.sum(comp_in[0:1, c : c + 1])
    for k in range(PIECES):
        out_copy(k).wait()


def local_step(sizes, density, design_mask, energy, decay, case_index, case_weight):
    n, ngx, ngy, lx, ly, lz, cells = sizes
    groups = lx // XG
    per = XG * ly
    others = ngx * ngy - 1
    dma = pltpu.SemaphoreType.DMA
    anywhere = pl.BlockSpec(memory_space=pltpu.HBM)
    smem = pl.BlockSpec(memory_space=pltpu.SMEM)
    vmem = pl.BlockSpec(memory_space=pltpu.VMEM)
    state = pltpu.VMEM((n, 8, lz), F32)
    sent = pltpu.VMEM((n, 8, lz), BF16)
    full, comp = pl.pallas_call(
        functools.partial(kernel, sizes),
        out_shape=(
            jax.ShapeDtypeStruct((lx, ly, lz), F32),
            jax.ShapeDtypeStruct((1, lz), F32),
        ),
        in_specs=[anywhere, anywhere, anywhere, vmem, smem, smem],
        out_specs=(vmem,) * 2,
        scratch_shapes=[
            pltpu.VMEM((lx, ly, lz), F32),
            pltpu.VMEM((lx, ly, lz), jnp.int32),
            pltpu.VMEM((CASES, lx, ly, lz), BF16),
            pltpu.VMEM((CASES, lz, lz), F32),
            pltpu.VMEM((groups, 2 * CASES, per, lz), BF16),
            pltpu.VMEM((2 * CASES * lz, 2 * lz), BF16),
            pltpu.VMEM((32, 2 * CASES * lz), BF16),
            pltpu.VMEM((lx + 2 * RADIUS, ly + 2 * YO, lz), F32),
            pltpu.VMEM((XG, ly + 2 * YO, lz), F32),
            pltpu.VMEM((lx, ly, lz), F32),
            state,
            pltpu.VMEM((32, lz), BF16),
            state,
            pltpu.VMEM((n + 4, 8, lz), F32),
            pltpu.VMEM((1, lz), F32),
            pltpu.VMEM((n, 1, lz), F32),
            state,
            state,
            sent,
            sent,
            state,
            sent,
            pltpu.VMEM((n + 4, 8, lz), BF16),
            pltpu.VMEM((n + 4, 8, lz), F32),
            pltpu.VMEM((n + 4, 8, lz), F32),
            pltpu.VMEM((1, lz), F32),
            pltpu.VMEM((others, 1, lz), F32),
            pltpu.VMEM((1, lz), F32),
            pltpu.VMEM((n, 1, lz), F32),
            pltpu.VMEM((RADIUS, ly, lz), BF16),
            pltpu.VMEM((RADIUS, ly, lz), BF16),
            pltpu.VMEM((2, RADIUS, lx, lz), BF16),
            pltpu.VMEM((2, RADIUS, lx, lz), BF16),
            pltpu.VMEM((2, RADIUS, RADIUS, lz), BF16),
            pltpu.VMEM((2, RADIUS, RADIUS, lz), BF16),
            pltpu.VMEM((2, 2, 8, lz), F32),
            pltpu.VMEM((2, 4, 8, lz), F32),
            pltpu.VMEM((2, 4, 8, lz), F32),
            dma((3, groups)),
            dma(()),
            dma(()),
            dma(()),
            dma(()),
            dma(()),
            dma(()),
            dma((others,)),
            dma((others,)),
            dma(()),
            dma(()),
            dma(()),
            dma(()),
            dma((2,)),
            dma((2,)),
            dma((2,)),
            dma((2,)),
            dma(()),
            dma(()),
            dma((2,)),
            dma((2,)),
            dma((2,)),
            dma((2,)),
        ],
        compiler_params=pltpu.CompilerParams(
            collective_id=0, has_side_effects=True, vmem_limit_bytes=40 * 1024 * 1024
        ),
        name="states",
    )(*(pltpu.with_memory_space_constraint(v, pltpu.HBM) for v in (density, design_mask, energy, decay, case_index, case_weight)))
    return pl.pallas_call(
        last,
        out_shape=(
            jax.ShapeDtypeStruct((lx, ly, lz), F32),
            jax.ShapeDtypeStruct((CASES,), F32),
        ),
        in_specs=[vmem] * 2,
        out_specs=(anywhere, smem),
        scratch_shapes=[dma((PIECES,))],
        compiler_params=pltpu.CompilerParams(vmem_limit_bytes=20 * 1024 * 1024),
        name="result",
    )(full, comp)


def solution(mesh):
    shape = mesh.shape
    n, ngx, ngy = shape["gz"], shape["gx"], shape["gy"]

    def whole(density, design_mask, energy, decay, case_index, case_weight):
        nx, ny, nz = density.shape
        sizes = (n, ngx, ngy, nx // ngx, ny // ngy, nz // n, nx * ny * nz)
        return jax.shard_map(
            functools.partial(local_step, sizes),
            mesh=mesh,
            in_specs=(
                P("gx", "gy", "gz"), P("gx", "gy", "gz"), P(None, "gx", "gy", "gz"), P(None, "gz"), P(), P(),
            ),
            out_specs=(P("gx", "gy", "gz"), P()),
            check_vma=False,
        )(density, design_mask, energy, decay, case_index, case_weight)

    return whole
```
